256 devices in a mesh: chain: 64 (over z, x, core), col: 4 (over y).
Axes of the slice: x: 4, y: 4, z: 8, core: 2. Of those that a mesh axis runs over, the one named last changes fastest.
Arguments:
- inverses: float32 [64, 2, 512, 512], P('chain', None, None, 'col'), may hold values from -3 to 3
- couplings: float32 [64, 2, 512, 512], P('chain', None, None, 'col'), may hold values from -3 to 3
- sources: float32 [64, 2, 512, 1024], P('chain', None, None, 'col'), may hold values from -6 to 6
- counts: int32 [64], P('chain'), may hold values from 384 to 512, as said below
Outputs:
- fields: float32 [64, 2, 512, 1024], P('chain', None, None, 'col')
The draws below stay inside these ranges and needn't reach their ends.
Inputs may be any that keep to these rules, and one draw needn't show every extreme that they name: `counts`: some slice has exactly 512 orbitals in use.
All inputs are finite; a program needn't handle non-finite values.
Results may differ from the reference program's by a relative error of at most 0.0003.
Values sent between devices are 32-bit elements; how exact they have to be, the bound alone decides.
A program may use at most 128 MiB of HBM per device.

```python
import math
import jax
import jax.numpy as jnp
from jax import lax

B = 512
SLICE_COUNT = 64
R = 1024


def rate_table(key):
    root_random_key = jax.random.fold_in(key, 7)
    category_key, quick_rate_key, spike_key, amplification_key = jax.random.split(root_random_key, 4)
    slow_share = 0.5
    sluggish_mask = jax.random.uniform(category_key, (B,)) < slow_share
    fast_rates = jax.random.uniform(quick_rate_key, (B,), minval=0.9, maxval=0.95)
    conduction_channel_rates = jnp.where(sluggish_mask, 0.975, fast_rates)
    spike_mask = jax.random.randint(spike_key, (SLICE_COUNT, 1), 0, 12) == 0
    spike_multiplier = jnp.where(spike_mask & sluggish_mask[None, :], 0.6, 1.0)
    per_slice_rates = conduction_channel_rates[None, :] * spike_multiplier
    slice_gains = jnp.exp(jax.random.uniform(amplification_key, (SLICE_COUNT, B), minval=-0.35, maxval=0.35))
    return (per_slice_rates, slice_gains)


def noisy_blocks(key, diagonal_values):
    noise_draw = jnp.clip(jax.random.normal(key, (SLICE_COUNT, 2, B, B)), -6.0, 6.0) * (0.08 / math.sqrt(B))
    identity_matrix = jnp.eye(B, dtype=jnp.float32)
    real_part = noise_draw[:, 0] + diagonal_values[:, :, None] * identity_matrix[None, :, :]
    return jnp.stack([real_part, noise_draw[:, 1]], axis=1).astype(jnp.float32)


def draw_inverses(key, part):
    per_slice_rates, slice_gains = rate_table(key)
    return noisy_blocks(jax.random.fold_in(key, 21), slice_gains)


def draw_couplings(key, part):
    per_slice_rates, slice_gains = rate_table(key)
    return noisy_blocks(jax.random.fold_in(key, 22), per_slice_rates / slice_gains)


def draw_counts(key, part):
    count_key = jax.random.fold_in(key, 5)
    drawn = jax.random.randint(count_key, (SLICE_COUNT,), 3 * B // 4, B + 1)
    chosen_slice = jax.random.randint(jax.random.fold_in(count_key, 1), (), 0, SLICE_COUNT)
    return jnp.where(jnp.arange(SLICE_COUNT) == chosen_slice, B, drawn).astype(jnp.int32)


def block_scale(key, dims, pieces, least, largest):
    loudness, own = 1.0, jax.random.fold_in(key, 6)
    for position, blocks in pieces:
        steps = jnp.exp(jax.random.uniform(jax.random.fold_in(own, position), (blocks,), jnp.float32, least / len(pieces), largest / len(pieces)))
        loudness = loudness * jnp.repeat(steps, dims[position] // blocks).reshape([-1 if axis == position else 1 for axis in range(len(dims))])
    return loudness


def centred(stream_key, shape, scale, bound, pieces=(), held_as=jnp.bfloat16):
    entries = jax.random.normal(stream_key, shape, jnp.float32) * scale
    if len(pieces) > 0:
        entries = block_scale(stream_key, shape, pieces, -0.22, 0.18) * entries
    return jnp.clip(entries, min=-bound, max=bound).astype(held_as)


def setup_inputs(seed: int = 0) -> dict:
    key_of = jax.random.split(jax.random.key(seed), 5)
    inverses = draw_inverses(jax.random.fold_in(key_of[4], 71), 0)
    couplings = draw_couplings(jax.random.fold_in(key_of[4], 71), 0)
    sources = centred(key_of[2], (SLICE_COUNT, 2, B, R), 1.0, 6.0, ((0, 64), (3, 4)), jnp.float32)
    counts = draw_counts(jax.random.fold_in(key_of[4], 71), 0)
    return dict(inverses=inverses, couplings=couplings, sources=sources, counts=counts)


def real_product(left_side, right_side):
    return jnp.dot(left_side, right_side, precision=lax.Precision.HIGHEST, preferred_element_type=jnp.float32)


def complex_product(left_side, right_side):
    real_part = real_product(left_side[0], right_side[0]) - real_product(left_side[1], right_side[1])
    imag_part = real_product(left_side[0], right_side[1]) + real_product(left_side[1], right_side[0])
    return jnp.stack([real_part, imag_part])


def reference(inverses, couplings, sources, counts):
    row_index = lax.iota(jnp.int32, B)

    def advance(carried_state, slice_items):
        inverse_block, coupling_block, source_block, active_count = slice_items
        active = (row_index < active_count).astype(jnp.float32)[:, None]
        updated = active * complex_product(inverse_block, source_block + complex_product(coupling_block, carried_state))
        return updated, updated

    zero_state = jnp.zeros((2, B, R), jnp.float32)
    final_state, all_fields = lax.scan(advance, zero_state, (inverses, couplings, sources, counts.astype(jnp.int32)))
    return all_fields
```

```python
import functools

import jax
import jax.numpy as jnp
from jax import lax
from jax.experimental import pallas as pl
from jax.experimental.pallas import tpu as pltpu
from jax.sharding import PartitionSpec as P

MESH = pl.DeviceIdType.MESH
PLANE = 8
ROWS = 4


def split(value):
    high = value.astype(jnp.bfloat16)
    return high, (value - high.astype(jnp.float32)).astype(jnp.bfloat16)


def product(real, imag, high_ref, low_ref):
    count, width = real.shape
    tile = min(256, width)
    real_high, real_low = split(real)
    imag_high, imag_low = split(imag)
    high = jnp.concatenate([real_high, imag_high], axis=0)
    both = jnp.concatenate([real_high, imag_high, real_low, imag_low], axis=0)

    def against(columns):
        wide = jnp.dot(both, high_ref[:, columns], preferred_element_type=jnp.float32)
        narrow = jnp.dot(high, low_ref[:, columns], preferred_element_type=jnp.float32)
        return wide[: 2 * count] + (wide[2 * count :] + narrow)

    reals, imags = [], []
    for start in range(0, width, tile):
        by_real = against(slice(start, start + tile))
        by_imag = against(slice(width + start, width + start + tile))
        reals.append(by_real[:count] - by_imag[count:])
        imags.append(by_imag[:count] + by_real[count:])
    return jnp.concatenate(reals, axis=1), jnp.concatenate(imags, axis=1)


def kernel(
    planes,
    inverse_ref,
    coupling_ref,
    source_ref,
    active_ref,
    out_ref,
    inv,
    cpl,
    src,
    inv_high,
    inv_low,
    own_high,
    own_low,
    pair_high,
    pair_low,
    even_map,
    even_in,
    even_offset,
    offset,
    map_in,
    map_out,
    off_in,
    off_out,
    whole,
    whole_high,
    whole_low,
    z_in,
    x_in,
    state,
    local_sem,
    gather_send,
    gather_recv,
    core_send,
    core_recv,
    map_send,
    map_recv,
    off_send,
    off_recv,
    z_recv,
    x_recv,
    out_send,
    pass_send,
):
    width = inv_high.shape[0]
    block = width // ROWS
    columns = offset.shape[0]
    map_step = block // map_recv.shape[0]
    off_step = columns // off_recv.shape[0]
    end_step = columns // z_recv.shape[0]

    place = lax.axis_index("chain")
    col = lax.axis_index("col")
    z = place // PLANE
    x = (place % PLANE) // 2
    core = place % 2
    up, down, across = (col + 1) % ROWS, (col + 3) % ROWS, (col + 2) % ROWS

    def at(z_to, x_to, core_to):
        return {"chain": z_to * PLANE + x_to * 2 + core_to, "col": col}

    partner = at(z, x, 1 - core)
    upward = {"chain": place, "col": up}
    downward = {"chain": place, "col": down}
    x_next, x_before = (x + 1) % 4, (x + 3) % 4
    z_next, z_before = (z + 1) % planes, (z + planes - 1) % planes

    barrier = pltpu.get_barrier_semaphore()
    greeted = (
        upward,
        downward,
        partner,
        at(z, x_next, core),
        at(z, x_before, core),
        at(z, x_next, 1 - core),
        at(z, x_before, 1 - core),
        at(z_next, x, core),
        at(z_before, x, core),
    )
    for device in greeted:
        pl.semaphore_signal(barrier, inc=1, device_id=device, device_id_type=MESH)
    pl.semaphore_wait(barrier, len(greeted))

    def remote(source, target, send, recv, device):
        return pltpu.make_async_remote_copy(
            src_ref=source,
            dst_ref=target,
            send_sem=send,
            recv_sem=recv,
            device_id=device,
            device_id_type=MESH,
        )

    def ring(own, held, which):
        send, recv = gather_send.at[which], gather_recv.at[which]
        first, second = held.at[:, 0], held.at[:, 1]
        own_first, own_second = own
        return [
            remote(own_first, first.at[col], send.at[0], recv.at[0], upward),
            remote(own_second, second.at[col], send.at[1], recv.at[1], downward),
            remote(own_second, second.at[col], send.at[2], recv.at[2], upward),
            remote(own_first, first.at[col], send.at[3], recv.at[3], downward),
            remote(first.at[down], first.at[down], send.at[4], recv.at[4], upward),
            remote(second.at[up], second.at[up], send.at[5], recv.at[5], downward),
        ]

    inv_ring = ring((inverse_ref.at[0, 0], inverse_ref.at[0, 1]), inv, 0)
    cpl_ring = ring((coupling_ref.at[0, 0], coupling_ref.at[0, 1]), cpl, 1)
    for copy in inv_ring[:4]:
        copy.start()
    own_inv = pltpu.make_async_copy(inverse_ref.at[0], inv.at[col], local_sem.at[0])
    own_cpl = pltpu.make_async_copy(coupling_ref.at[0], cpl.at[col], local_sem.at[1])
    own_src = pltpu.make_async_copy(source_ref.at[0], src, local_sem.at[2])
    own_inv.start()
    own_cpl.start()
    own_src.start()

    active = active_ref[0:1, :]

    def take_inverse(which):
        rows = pl.ds(pl.multiple_of(which * block, block), block)
        for part in range(2):
            high, low = split(inv[which, part].T * active)
            inv_high[rows, part * width : (part + 1) * width] = high
            inv_low[rows, part * width : (part + 1) * width] = low

    own_inv.wait()
    take_inverse(col)
    inv_ring[0].wait_recv()
    inv_ring[4].start()
    inv_ring[1].wait_recv()
    inv_ring[5].start()
    for copy in cpl_ring[:4]:
        copy.start()
    inv_ring[2].wait_recv()
    take_inverse(down)
    inv_ring[3].wait_recv()
    take_inverse(up)
    inv_ring[4].wait_recv()
    inv_ring[5].wait_recv()
    take_inverse(across)

    own_src.wait()
    for start in range(0, columns, block):
        real, imag = product(
            src[0, :, start : start + block].T, src[1, :, start : start + block].T, inv_high, inv_low
        )
        offset[start : start + block, :width] = real
        offset[start : start + block, width:] = imag

    even_offset_copy = remote(offset, even_offset, core_send.at[ROWS], core_recv.at[ROWS], partner)

    @pl.when(core == 0)
    def _():
        even_offset_copy.start()

    def even_map_copy(which):
        return remote(
            even_map.at[which], even_in.at[which], core_send.at[which], core_recv.at[which], partner
        )

    def take_coupling(which):
        rows = pl.ds(pl.multiple_of(which * block, block), block)
        real, imag = product(cpl[which, 0].T, cpl[which, 1].T, inv_high, inv_low)
        for part, value in enumerate((real, imag)):
            high, low = split(value)
            own_high[rows, part * width : (part + 1) * width] = high
            own_low[rows, part * width : (part + 1) * width] = low

        @pl.when(core == 0)
        def _():
            even_map[which, :, :width] = real
            even_map[which, :, width:] = imag
            even_map_copy(which).start()

    own_cpl.wait()
    take_coupling(col)
    cpl_ring[0].wait_recv()
    cpl_ring[4].start()
    cpl_ring[1].wait_recv()
    cpl_ring[5].start()
    cpl_ring[2].wait_recv()
    take_coupling(down)
    cpl_ring[3].wait_recv()
    take_coupling(up)
    cpl_ring[4].wait_recv()
    cpl_ring[5].wait_recv()
    take_coupling(across)
    for copy in inv_ring + cpl_ring:
        copy.wait_send()

    def rows_of(step, index):
        return pl.ds(pl.multiple_of(index * step, step), step)

    def chunk(ref, rows):
        return ref[rows, :width], ref[rows, width:]

    def put(ref, rows, value):
        ref[rows, :width] = value[0]
        ref[rows, width:] = value[1]

    def plus(value, other):
        return value[0] + other[0], value[1] + other[1]

    next_odd = at(z, x_next, 1)

    def map_copy(index):
        rows = rows_of(map_step, index)
        return remote(
            map_out.at[rows], map_in.at[rows], map_send.at[index], map_recv.at[index], next_odd
        )

    def off_copy(index):
        rows = rows_of(off_step, index)
        return remote(
            off_out.at[rows], off_in.at[rows], off_send.at[index], off_recv.at[index], next_odd
        )

    whole_ring = ring((map_out.at[:, :width], map_out.at[:, width:]), whole, 2)

    @pl.when(core == 1)
    def _():
        def compose(which):
            rows = pl.ds(pl.multiple_of(which * block, block), block)
            even_map_copy(which).wait_recv()
            value = product(even_in[which, :, :width], even_in[which, :, width:], own_high, own_low)
            for part in range(2):
                high, low = split(value[part])
                pair_high[rows, part * width : (part + 1) * width] = high
                pair_low[rows, part * width : (part + 1) * width] = low
            return value

        first = compose(col)

        @pl.when(x == 0)
        def _():
            put(map_out, slice(None), first)
            for index in range(map_recv.shape[0]):
                map_copy(index).start()

        for which in (down, up, across):
            compose(which)
        even_offset_copy.wait_recv()

        def compose_offset(index, carry):
            rows = rows_of(block, index)
            value = product(*chunk(even_offset, rows), own_high, own_low)
            put(offset, rows, plus(value, chunk(offset, rows)))
            return carry

        lax.fori_loop(0, columns // block, compose_offset, 0)

        @pl.when(x == 0)
        def _():
            off_out[...] = offset[...]
            for index in range(off_recv.shape[0]):
                off_copy(index).start()

        @pl.when(x > 0)
        def _():
            def map_sweep(index, carry):
                rows = rows_of(map_step, index)
                map_copy(index).wait_recv()
                put(map_out, rows, product(*chunk(map_in, rows), pair_high, pair_low))

                @pl.when(x < 3)
                def _():
                    map_copy(index).start()

                return carry

            lax.fori_loop(0, map_recv.shape[0], map_sweep, 0)

            def off_sweep(index, carry):
                rows = rows_of(off_step, index)
                off_copy(index).wait_recv()
                value = product(*chunk(off_in, rows), pair_high, pair_low)
                put(off_out, rows, plus(value, chunk(offset, rows)))

                @pl.when(x < 3)
                def _():
                    off_copy(index).start()

                return carry

            @pl.when(x == 3)
            def _():
                for copy in whole_ring[:4]:
                    copy.start()

            lax.fori_loop(0, off_recv.shape[0] // 2, off_sweep, 0)

            @pl.when(x == 3)
            def _():
                whole_ring[0].wait_recv()
                whole_ring[4].start()
                whole_ring[1].wait_recv()
                whole_ring[5].start()

            lax.fori_loop(off_recv.shape[0] // 2, off_recv.shape[0], off_sweep, 0)

        @pl.when(x < 3)
        def _():
            for index in range(map_recv.shape[0]):
                map_copy(index).wait_send()
            for index in range(off_recv.shape[0]):
                off_copy(index).wait_send()

    ends = z_recv.shape[0]

    def z_copy(index):
        rows = rows_of(end_step, index)
        return remote(
            state.at[rows], z_in.at[rows], out_send.at[index], z_recv.at[index], at(z_next, 3, 1)
        )

    def enter_copy(index):
        rows = rows_of(end_step, index)
        return remote(
            z_in.at[rows], x_in.at[rows], pass_send.at[index], x_recv.at[index], at(z, 0, 1)
        )

    def x_copy(index):
        rows = rows_of(end_step, index)
        device = at(z, x_next, jnp.where(x_next == 3, 0, 1))
        return remote(state.at[rows], x_in.at[rows], out_send.at[index], x_recv.at[index], device)

    def pass_copy(index):
        rows = rows_of(end_step, index)
        return remote(
            x_in.at[rows], x_in.at[rows], pass_send.at[index], x_recv.at[index], partner
        )

    @pl.when((core == 1) & (x == 3))
    def _():
        @pl.when(z == 0)
        def _():
            z_in[...] = jnp.zeros_like(z_in)
            state[...] = off_out[...]
            for index in range(ends):
                z_copy(index).start()
            for index in range(ends):
                enter_copy(index).start()

        def take_whole(which):
            rows = pl.ds(pl.multiple_of(which * block, block), block)
            for part in range(2):
                high, low = split(whole[which, part])
                whole_high[rows, part * width : (part + 1) * width] = high
                whole_low[rows, part * width : (part + 1) * width] = low

        for part in range(2):
            whole[col, part] = map_out[:, part * width : (part + 1) * width]
        take_whole(col)
        whole_ring[2].wait_recv()
        take_whole(down)
        whole_ring[3].wait_recv()
        take_whole(up)
        whole_ring[4].wait_recv()
        whole_ring[5].wait_recv()
        take_whole(across)
        for copy in whole_ring:
            copy.wait_send()

        @pl.when(z > 0)
        def _():
            def z_sweep(index, carry):
                rows = rows_of(end_step, index)
                z_copy(index).wait_recv()
                enter_copy(index).start()
                value = product(*chunk(z_in, rows), whole_high, whole_low)
                put(state, rows, plus(value, chunk(off_out, rows)))

                @pl.when(z < planes - 1)
                def _():
                    z_copy(index).start()

                return carry

            lax.fori_loop(0, ends, z_sweep, 0)

        @pl.when(z < planes - 1)
        def _():
            for index in range(ends):
                z_copy(index).wait_send()

        for index in range(ends):
            enter_copy(index).wait_send()

    @pl.when((core == 1) & (x < 3))
    def _():
        def x_sweep(index, carry):
            rows = rows_of(end_step, index)
            x_copy(index).wait_recv()
            pass_copy(index).start()
            value = product(*chunk(x_in, rows), pair_high, pair_low)
            put(state, rows, plus(value, chunk(offset, rows)))
            x_copy(index).start()
            return carry

        lax.fori_loop(0, ends, x_sweep, 0)
        for index in range(ends):
            x_copy(index).wait_send()
            pass_copy(index).wait_send()

    @pl.when(core == 0)
    def _():
        def even_sweep(index, carry):
            rows = rows_of(end_step, index)
            x_copy(index).wait_recv()
            value = product(*chunk(x_in, rows), own_high, own_low)
            put(state, rows, plus(value, chunk(offset, rows)))
            return carry

        lax.fori_loop(0, ends, even_sweep, 0)
        for which in range(ROWS):
            even_map_copy(which).wait_send()
        even_offset_copy.wait_send()

    for start in range(0, columns, block):
        for part in range(2):
            out_ref[0, part, :, start : start + block] = state[
                start : start + block, part * width : (part + 1) * width
            ].T


def local(planes, inverses, couplings, sources, counts):
    width, block = inverses.shape[2], inverses.shape[3]
    columns = sources.shape[3]
    active = (lax.iota(jnp.int32, width) < counts[0]).astype(jnp.float32)
    active = jnp.broadcast_to(active[None], (8, width))
    map_chunks, off_chunks, end_chunks = 4, 8, 8
    single, half = jnp.float32, jnp.bfloat16
    vmem, dma = pltpu.VMEM, pltpu.SemaphoreType.DMA
    held_map = vmem((width, 2 * width), half)
    rows_buffer = vmem((columns, 2 * width), single)
    map_buffer = vmem((block, 2 * width), single)
    any_space = pl.BlockSpec(memory_space=pl.ANY)
    in_vmem = pl.BlockSpec(memory_space=pltpu.VMEM)
    return pl.pallas_call(
        functools.partial(kernel, planes),
        out_shape=jax.ShapeDtypeStruct(sources.shape, single),
        in_specs=[any_space, any_space, any_space, in_vmem],
        out_specs=in_vmem,
        scratch_shapes=[
            vmem((ROWS, 2, width, block), single),
            vmem((ROWS, 2, width, block), single),
            vmem((2, width, columns), single),
            held_map,
            held_map,
            held_map,
            held_map,
            held_map,
            held_map,
            vmem((ROWS, block, 2 * width), single),
            vmem((ROWS, block, 2 * width), single),
            rows_buffer,
            rows_buffer,
            map_buffer,
            map_buffer,
            rows_buffer,
            rows_buffer,
            vmem((ROWS, 2, block, width), single),
            held_map,
            held_map,
            rows_buffer,
            rows_buffer,
            rows_buffer,
            dma((3,)),
            dma((3, 6)),
            dma((3, 6)),
            dma((ROWS + 1,)),
            dma((ROWS + 1,)),
            dma((map_chunks,)),
            dma((map_chunks,)),
            dma((off_chunks,)),
            dma((off_chunks,)),
            dma((end_chunks,)),
            dma((end_chunks,)),
            dma((end_chunks,)),
            dma((end_chunks,)),
        ],
        compiler_params=pltpu.CompilerParams(
            collective_id=0, has_side_effects=True, vmem_limit_bytes=60 * 2**20
        ),
    )(inverses, couplings, sources, active)


def solution(mesh):
    placed = (
        P("chain", None, None, "col"),
        P("chain", None, None, "col"),
        P("chain", None, None, "col"),
        P("chain"),
    )
    return jax.shard_map(
        functools.partial(local, mesh.shape["chain"] // PLANE),
        mesh=mesh,
        in_specs=placed,
        out_specs=P("chain", None, None, "col"),
        check_vma=False,
    )
```

```python
import functools

import jax
import jax.numpy as jnp
from jax import lax
from jax.experimental import pallas as pl
from jax.experimental.pallas import tpu as pltpu
from jax.sharding import PartitionSpec as P

MESH = pl.DeviceIdType.MESH
PLANE = 8
ROWS = 4


def split(value):
    high = value.astype(jnp.bfloat16)
    return high, (value - high.astype(jnp.float32)).astype(jnp.bfloat16)


def product(real, imag, high_ref, low_ref):
    count, width = real.shape
    tile = min(256, width)
    real_high, real_low = split(real)
    imag_high, imag_low = split(imag)
    high = jnp.concatenate([real_high, imag_high], axis=0)
    both = jnp.concatenate([real_high, imag_high, real_low, imag_low], axis=0)

    def against(columns):
        wide = jnp.dot(both, high_ref[:, columns], preferred_element_type=jnp.float32)
        narrow = jnp.dot(high, low_ref[:, columns], preferred_element_type=jnp.float32)
        return wide[: 2 * count] + (wide[2 * count :] + narrow)

    reals, imags = [], []
    for start in range(0, width, tile):
        by_real = against(slice(start, start + tile))
        by_imag = against(slice(width + start, width + start + tile))
        reals.append(by_real[:count] - by_imag[count:])
        imags.append(by_imag[:count] + by_real[count:])
    return jnp.concatenate(reals, axis=1), jnp.concatenate(imags, axis=1)


def kernel(
    planes,
    inverse_ref,
    coupling_ref,
    source_ref,
    count_ref,
    out_ref,
    inv,
    cpl,
    src,
    inv_high,
    inv_low,
    own_high,
    own_low,
    pair_high,
    pair_low,
    even_map,
    even_in,
    even_offset,
    offset,
    map_in,
    map_out,
    off_in,
    off_out,
    whole,
    whole_high,
    whole_low,
    z_in,
    x_in,
    state,
    local_sem,
    gather_send,
    gather_recv,
    core_send,
    core_recv,
    map_send,
    map_recv,
    off_send,
    off_recv,
    z_recv,
    x_recv,
    out_send,
    pass_send,
    back_send,
    whole_send,
    whole_recv,
    turn_sem,
):
    width = inv_high.shape[0]
    block = width // ROWS
    columns = offset.shape[0]
    map_step = block // map_recv.shape[0]
    off_step = columns // off_recv.shape[0]
    end_step = columns // z_recv.shape[0]

    place = lax.axis_index("chain")
    col = lax.axis_index("col")
    z = place // PLANE
    x = (place % PLANE) // 2
    core = place % 2
    up, down, across = (col + 1) % ROWS, (col + 3) % ROWS, (col + 2) % ROWS

    def at(z_to, x_to, core_to):
        return {"chain": z_to * PLANE + x_to * 2 + core_to, "col": col}

    partner = at(z, x, 1 - core)
    upward = {"chain": place, "col": up}
    downward = {"chain": place, "col": down}
    x_next, x_before = (x + 1) % 4, (x + 3) % 4
    odd, last = core == 1, (core == 1) & (x == 3)

    barrier = pltpu.get_barrier_semaphore()

    def greet(when, device):
        @pl.when(when)
        def _():
            pl.semaphore_signal(barrier, inc=1, device_id=device, device_id_type=MESH)

        return jnp.where(when, 1, 0)

    for device in (upward, downward, partner):
        pl.semaphore_signal(barrier, inc=1, device_id=device, device_id_type=MESH)
    greeted = 3
    greeted += greet(odd, at(z, x_next, 1))
    greeted += greet(odd, at(z, x_before, 1))
    greeted += greet(odd & (x < 3), at(z, x_next, 0))
    greeted += greet((core == 0) & (x > 0), at(z, x_before, 1))
    greeted += greet(last & (z < planes - 1), at(z + 1, 3, 1))
    greeted += greet(last & (z > 0), at(z - 1, 3, 1))
    pl.semaphore_wait(barrier, greeted)

    def remote(source, target, send, recv, device):
        return pltpu.make_async_remote_copy(
            src_ref=source,
            dst_ref=target,
            send_sem=send,
            recv_sem=recv,
            device_id=device,
            device_id_type=MESH,
        )

    def ring(own, held, which):
        send, recv = gather_send.at[which], gather_recv.at[which]
        first, second = held.at[:, 0], held.at[:, 1]
        own_first, own_second = own
        return [
            remote(own_first, first.at[col], send.at[0], recv.at[0], upward),
            remote(own_second, second.at[col], send.at[1], recv.at[1], downward),
            remote(own_second, second.at[col], send.at[2], recv.at[2], upward),
            remote(own_first, first.at[col], send.at[3], recv.at[3], downward),
            remote(first.at[down], first.at[down], send.at[4], recv.at[4], upward),
            remote(second.at[up], second.at[up], send.at[5], recv.at[5], downward),
        ]

    inv_ring = ring((inverse_ref.at[0, 0], inverse_ref.at[0, 1]), inv, 0)
    cpl_ring = ring((coupling_ref.at[0, 0], coupling_ref.at[0, 1]), cpl, 1)
    own_inv = pltpu.make_async_copy(inverse_ref.at[0], inv.at[col], local_sem.at[0])
    own_cpl = pltpu.make_async_copy(coupling_ref.at[0], cpl.at[col], local_sem.at[1])
    own_src = pltpu.make_async_copy(source_ref.at[0], src, local_sem.at[2])
    own_inv.start()
    own_cpl.start()
    own_src.start()

    @pl.when(core == 0)
    def _():
        pl.semaphore_wait(turn_sem, 1)

    for copy in inv_ring[:4]:
        copy.start()

    active = (lax.broadcasted_iota(jnp.int32, (1, width), 1) < count_ref[0]).astype(jnp.float32)

    def take_inverse(which):
        rows = pl.ds(pl.multiple_of(which * block, block), block)
        for part in range(2):
            high, low = split(inv[which, part].T * active)
            inv_high[rows, part * width : (part + 1) * width] = high
            inv_low[rows, part * width : (part + 1) * width] = low

    own_inv.wait()
    take_inverse(col)
    inv_ring[0].wait_recv()
    inv_ring[4].start()
    inv_ring[1].wait_recv()
    inv_ring[5].start()
    for copy in cpl_ring[:4]:
        copy.start()
    inv_ring[2].wait_recv()
    take_inverse(down)
    inv_ring[3].wait_recv()
    take_inverse(up)
    inv_ring[4].wait_recv()
    inv_ring[5].wait_recv()
    take_inverse(across)

    def even_map_copy(which):
        return remote(
            even_map.at[which], even_in.at[which], core_send.at[which], core_recv.at[which], partner
        )

    def take_coupling(which):
        rows = pl.ds(pl.multiple_of(which * block, block), block)
        real, imag = product(cpl[which, 0].T, cpl[which, 1].T, inv_high, inv_low)
        for part, value in enumerate((real, imag)):
            high, low = split(value)
            own_high[rows, part * width : (part + 1) * width] = high
            own_low[rows, part * width : (part + 1) * width] = low

        @pl.when(core == 0)
        def _():
            even_map[which, :, :width] = real
            even_map[which, :, width:] = imag
            even_map_copy(which).start()

    own_cpl.wait()
    take_coupling(col)
    own_src.wait()
    for start in range(0, columns, block):
        real, imag = product(
            src[0, :, start : start + block].T, src[1, :, start : start + block].T, inv_high, inv_low
        )
        offset[start : start + block, :width] = real
        offset[start : start + block, width:] = imag

    even_offset_copy = remote(offset, even_offset, core_send.at[ROWS], core_recv.at[ROWS], partner)

    @pl.when(core == 0)
    def _():
        even_offset_copy.start()

    cpl_ring[0].wait_recv()
    cpl_ring[4].start()
    cpl_ring[1].wait_recv()
    cpl_ring[5].start()
    cpl_ring[2].wait_recv()
    cpl_ring[3].wait_recv()

    @pl.when(core == 1)
    def _():
        pl.semaphore_signal(turn_sem, inc=1, device_id=partner, device_id_type=MESH)

    take_coupling(down)
    take_coupling(up)
    cpl_ring[4].wait_recv()
    cpl_ring[5].wait_recv()
    take_coupling(across)
    for copy in inv_ring + cpl_ring:
        copy.wait_send()

    def rows_of(step, index):
        return pl.ds(pl.multiple_of(index * step, step), step)

    def chunk(ref, rows):
        return ref[rows, :width], ref[rows, width:]

    def put(ref, rows, value):
        ref[rows, :width] = value[0]
        ref[rows, width:] = value[1]

    def plus(value, other):
        return value[0] + other[0], value[1] + other[1]

    next_odd = at(z, x_next, 1)

    def map_copy(index):
        rows = rows_of(map_step, index)
        return remote(
            map_out.at[rows], map_in.at[rows], map_send.at[index], map_recv.at[index], next_odd
        )

    def off_copy(index):
        rows = rows_of(off_step, index)
        return remote(
            off_out.at[rows], off_in.at[rows], off_send.at[index], off_recv.at[index], next_odd
        )

    maps = map_recv.shape[0]

    def whole_copy(kind, index):
        rows = rows_of(map_step, index)
        send, recv = whole_send.at[kind, index], whole_recv.at[kind, index]
        if kind < 2:
            return remote(map_out.at[rows], whole.at[col, rows], send, recv, (upward, downward)[kind])
        if index < maps // 2:
            return remote(whole.at[down, rows], whole.at[down, rows], send, recv, upward)
        return remote(whole.at[up, rows], whole.at[up, rows], send, recv, downward)

    def forward(index):
        whole_copy(0 if index < maps // 2 else 1, index).wait_recv()
        whole_copy(2, index).start()

    @pl.when(core == 1)
    def _():
        def compose(which):
            rows = pl.ds(pl.multiple_of(which * block, block), block)
            even_map_copy(which).wait_recv()
            value = product(even_in[which, :, :width], even_in[which, :, width:], own_high, own_low)
            for part in range(2):
                high, low = split(value[part])
                pair_high[rows, part * width : (part + 1) * width] = high
                pair_low[rows, part * width : (part + 1) * width] = low
            return value

        first = compose(col)

        @pl.when(x == 0)
        def _():
            put(map_out, slice(None), first)
            for index in range(map_recv.shape[0]):
                map_copy(index).start()

        even_offset_copy.wait_recv()

        def compose_offset(index, carry):
            rows = rows_of(block, index)
            value = product(*chunk(even_offset, rows), own_high, own_low)
            put(offset, rows, plus(value, chunk(offset, rows)))
            return carry

        lax.fori_loop(0, columns // block, compose_offset, 0)

        @pl.when(x == 0)
        def _():
            off_out[...] = offset[...]
            for index in range(off_recv.shape[0]):
                off_copy(index).start()

        for which in (down, up, across):
            compose(which)

        @pl.when(x > 0)
        def _():
            def map_sweep(index, carry):
                rows = rows_of(map_step, index)
                map_copy(index).wait_recv()
                put(map_out, rows, product(*chunk(map_in, rows), pair_high, pair_low))

                @pl.when(x < 3)
                def _():
                    map_copy(index).start()

                @pl.when(x == 3)
                def _():
                    whole_copy(0, index).start()
                    whole_copy(1, index).start()

                return carry

            lax.fori_loop(0, map_recv.shape[0], map_sweep, 0)

            def off_sweep(index, carry):
                rows = rows_of(off_step, index)
                off_copy(index).wait_recv()
                value = product(*chunk(off_in, rows), pair_high, pair_low)
                put(off_out, rows, plus(value, chunk(offset, rows)))

                @pl.when(x < 3)
                def _():
                    off_copy(index).start()

                return carry

            done = 0
            for index in range(maps):
                until = max(0, 2 * index - maps // 2)
                if until > done:
                    lax.fori_loop(done, until, off_sweep, 0)
                    done = until

                @pl.when(x == 3)
                def _():
                    forward(index)

            lax.fori_loop(done, off_recv.shape[0], off_sweep, 0)

        @pl.when(x < 3)
        def _():
            for index in range(maps):
                whole_copy(0, index).start()
                whole_copy(1, index).start()
            for index in range(maps):
                forward(index)
            for index in range(map_recv.shape[0]):
                map_copy(index).wait_send()
            for index in range(off_recv.shape[0]):
                off_copy(index).wait_send()

        def take_whole(which):
            rows = pl.ds(pl.multiple_of(which * block, block), block)
            high, low = split(whole[which])
            whole_high[rows] = high
            whole_low[rows] = low

        whole[col] = map_out[...]
        take_whole(col)
        for index in range(maps // 2, maps):
            whole_copy(0, index).wait_recv()
        take_whole(down)
        for index in range(maps // 2):
            whole_copy(1, index).wait_recv()
        take_whole(up)
        for index in range(maps):
            whole_copy(2, index).wait_recv()
        take_whole(across)
        for kind in range(3):
            for index in range(maps):
                whole_copy(kind, index).wait_send()

    ends = z_recv.shape[0]

    def z_copy(index):
        rows = rows_of(end_step, index)
        return remote(
            state.at[rows], z_in.at[rows], out_send.at[index], z_recv.at[index], at((z + 1) % planes, 3, 1)
        )

    def enter_copy(index):
        rows = rows_of(end_step, index)
        return remote(
            z_in.at[rows], x_in.at[rows], pass_send.at[index], x_recv.at[index], at(z, 0, 1)
        )

    def enter_back_copy(index):
        rows = rows_of(end_step, index)
        return remote(
            z_in.at[rows], x_in.at[rows], back_send.at[index], x_recv.at[index], at(z, 2, 1)
        )

    def back_copy(index):
        rows = rows_of(end_step, index)
        return remote(
            x_in.at[rows], x_in.at[rows], back_send.at[index], x_recv.at[index], at(z, x_before, 1)
        )

    def pass_copy(index):
        rows = rows_of(end_step, index)
        return remote(
            x_in.at[rows], x_in.at[rows], pass_send.at[index], x_recv.at[index], partner
        )

    def x_copy(index):
        rows = rows_of(end_step, index)
        return remote(
            state.at[rows], x_in.at[rows], out_send.at[index], x_recv.at[index], at(z, x_next, 0)
        )

    @pl.when((core == 1) & (x == 3))
    def _():
        @pl.when(z == 0)
        def _():
            z_in[...] = jnp.zeros_like(z_in)
            state[...] = off_out[...]
            for index in range(ends):
                z_copy(index).start()
            for index in range(ends):
                enter_copy(index).start()
                enter_back_copy(index).start()

        @pl.when(z > 0)
        def _():
            def z_sweep(index, carry):
                rows = rows_of(end_step, index)
                z_copy(index).wait_recv()
                enter_copy(index).start()
                enter_back_copy(index).start()
                value = product(*chunk(z_in, rows), whole_high, whole_low)
                put(state, rows, plus(value, chunk(off_out, rows)))

                @pl.when(z < planes - 1)
                def _():
                    z_copy(index).start()

                return carry

            lax.fori_loop(0, ends, z_sweep, 0)

        @pl.when(z < planes - 1)
        def _():
            for index in range(ends):
                z_copy(index).wait_send()

        for index in range(ends):
            enter_copy(index).wait_send()
            enter_back_copy(index).wait_send()

    @pl.when((core == 1) & (x < 3))
    def _():
        def x_sweep(index, carry):
            rows = rows_of(end_step, index)
            x_copy(index).wait_recv()

            @pl.when(x == 2)
            def _():
                back_copy(index).start()

            @pl.when(x == 0)
            def _():
                pass_copy(index).start()

            value = product(*chunk(x_in, rows), whole_high, whole_low)
            put(state, rows, plus(value, chunk(off_out, rows)))
            x_copy(index).start()
            return carry

        lax.fori_loop(0, ends, x_sweep, 0)
        for index in range(ends):
            x_copy(index).wait_send()

        @pl.when(x == 2)
        def _():
            for index in range(ends):
                back_copy(index).wait_send()

        @pl.when(x == 0)
        def _():
            for index in range(ends):
                pass_copy(index).wait_send()

    @pl.when(core == 0)
    def _():
        def even_sweep(index, carry):
            rows = rows_of(end_step, index)
            x_copy(index).wait_recv()
            value = product(*chunk(x_in, rows), own_high, own_low)
            put(state, rows, plus(value, chunk(offset, rows)))
            return carry

        lax.fori_loop(0, ends, even_sweep, 0)
        for which in range(ROWS):
            even_map_copy(which).wait_send()
        even_offset_copy.wait_send()

    for start in range(0, columns, block):
        for part in range(2):
            out_ref[0, part, :, start : start + block] = state[
                start : start + block, part * width : (part + 1) * width
            ].T


def local(planes, inverses, couplings, sources, counts):
    width, block = inverses.shape[2], inverses.shape[3]
    columns = sources.shape[3]
    map_chunks, off_chunks, end_chunks = 4, 16, 16
    single, half = jnp.float32, jnp.bfloat16
    vmem, dma = pltpu.VMEM, pltpu.SemaphoreType.DMA
    held_map = vmem((width, 2 * width), half)
    rows_buffer = vmem((columns, 2 * width), single)
    map_buffer = vmem((block, 2 * width), single)
    any_space = pl.BlockSpec(memory_space=pl.ANY)
    in_vmem = pl.BlockSpec(memory_space=pltpu.VMEM)
    return pl.pallas_call(
        functools.partial(kernel, planes),
        out_shape=jax.ShapeDtypeStruct(sources.shape, single),
        in_specs=[any_space, any_space, any_space, pl.BlockSpec(memory_space=pltpu.SMEM)],
        out_specs=in_vmem,
        scratch_shapes=[
            vmem((ROWS, 2, width, block), single),
            vmem((ROWS, 2, width, block), single),
            vmem((2, width, columns), single),
            held_map,
            held_map,
            held_map,
            held_map,
            held_map,
            held_map,
            vmem((ROWS, block, 2 * width), single),
            vmem((ROWS, block, 2 * width), single),
            rows_buffer,
            rows_buffer,
            map_buffer,
            map_buffer,
            rows_buffer,
            rows_buffer,
            vmem((ROWS, block, 2 * width), single),
            held_map,
            held_map,
            rows_buffer,
            rows_buffer,
            rows_buffer,
            dma((3,)),
            dma((2, 6)),
            dma((2, 6)),
            dma((ROWS + 1,)),
            dma((ROWS + 1,)),
            dma((map_chunks,)),
            dma((map_chunks,)),
            dma((off_chunks,)),
            dma((off_chunks,)),
            dma((end_chunks,)),
            dma((end_chunks,)),
            dma((end_chunks,)),
            dma((end_chunks,)),
            dma((end_chunks,)),
            dma((3, map_chunks)),
            dma((3, map_chunks)),
            pltpu.SemaphoreType.REGULAR,
        ],
        compiler_params=pltpu.CompilerParams(
            collective_id=0, has_side_effects=True, vmem_limit_bytes=40 * 2**20
        ),
    )(inverses, couplings, sources, counts)


def solution(mesh):
    placed = (
        P("chain", None, None, "col"),
        P("chain", None, None, "col"),
        P("chain", None, None, "col"),
        P("chain"),
    )
    return jax.shard_map(
        functools.partial(local, mesh.shape["chain"] // PLANE),
        mesh=mesh,
        in_specs=placed,
        out_specs=P("chain", None, None, "col"),
        check_vma=False,
    )
```

```python
import functools

import jax
import jax.numpy as jnp
from jax import lax
from jax.experimental import pallas as pl
from jax.experimental.pallas import tpu as pltpu
from jax.sharding import PartitionSpec as P

MESH = pl.DeviceIdType.MESH
PLANE = 8
ROWS = 4


def split(value):
    high = value.astype(jnp.bfloat16)
    return high, (value - high.astype(jnp.float32)).astype(jnp.bfloat16)


def product(real, imag, high_ref, low_ref):
    count, width = real.shape
    tile = min(256, width)
    real_high, real_low = split(real)
    imag_high, imag_low = split(imag)
    high = jnp.concatenate([real_high, imag_high], axis=0)
    both = jnp.concatenate([real_high, imag_high, real_low, imag_low], axis=0)

    def against(columns):
        wide = jnp.dot(both, high_ref[:, columns], preferred_element_type=jnp.float32)
        narrow = jnp.dot(high, low_ref[:, columns], preferred_element_type=jnp.float32)
        return wide[: 2 * count] + (wide[2 * count :] + narrow)

    reals, imags = [], []
    for start in range(0, width, tile):
        by_real = against(slice(start, start + tile))
        by_imag = against(slice(width + start, width + start + tile))
        reals.append(by_real[:count] - by_imag[count:])
        imags.append(by_imag[:count] + by_real[count:])
    return jnp.concatenate(reals, axis=1), jnp.concatenate(imags, axis=1)


def kernel(
    planes,
    inverse_ref,
    coupling_ref,
    source_ref,
    count_ref,
    out_ref,
    inv,
    cpl,
    src,
    inv_high,
    inv_low,
    own_high,
    own_low,
    pair_high,
    pair_low,
    even_map,
    even_in,
    even_offset,
    offset,
    map_in,
    map_out,
    off_in,
    off_out,
    whole,
    whole_high,
    whole_low,
    z_in,
    x_in,
    state,
    local_sem,
    gather_send,
    gather_recv,
    core_send,
    core_recv,
    map_send,
    map_recv,
    off_send,
    off_recv,
    z_recv,
    x_recv,
    out_send,
    pass_send,
    back_send,
    whole_send,
    whole_recv,
    turn_sem,
):
    width = inv_high.shape[0]
    block = width // ROWS
    columns = offset.shape[0]
    map_step = block // map_recv.shape[0]
    off_step = columns // off_recv.shape[0]
    end_step = columns // z_recv.shape[0]

    place = lax.axis_index("chain")
    col = lax.axis_index("col")
    z = place // PLANE
    x = (place % PLANE) // 2
    core = place % 2
    up, down, across = (col + 1) % ROWS, (col + 3) % ROWS, (col + 2) % ROWS

    def at(z_to, x_to, core_to):
        return {"chain": z_to * PLANE + x_to * 2 + core_to, "col": col}

    partner = at(z, x, 1 - core)
    upward = {"chain": place, "col": up}
    downward = {"chain": place, "col": down}
    x_next, x_before = (x + 1) % 4, (x + 3) % 4
    odd, last = core == 1, (core == 1) & (x == 3)

    barrier = pltpu.get_barrier_semaphore()

    def greet(when, device):
        @pl.when(when)
        def _():
            pl.semaphore_signal(barrier, inc=1, device_id=device, device_id_type=MESH)

        return jnp.where(when, 1, 0)

    for device in (upward, downward, partner):
        pl.semaphore_signal(barrier, inc=1, device_id=device, device_id_type=MESH)
    greeted = 3
    greeted += greet(odd, at(z, x_next, 1))
    greeted += greet(odd, at(z, x_before, 1))
    greeted += greet(odd & (x < 3), at(z, x_next, 0))
    greeted += greet((core == 0) & (x > 0), at(z, x_before, 1))
    greeted += greet(last & (z < planes - 1), at(z + 1, 3, 1))
    greeted += greet(last & (z > 0), at(z - 1, 3, 1))
    pl.semaphore_wait(barrier, greeted)

    def remote(source, target, send, recv, device):
        return pltpu.make_async_remote_copy(
            src_ref=source,
            dst_ref=target,
            send_sem=send,
            recv_sem=recv,
            device_id=device,
            device_id_type=MESH,
        )

    def ring(own, held, which):
        send, recv = gather_send.at[which], gather_recv.at[which]
        first, second = held.at[:, 0], held.at[:, 1]
        own_first, own_second = own
        return [
            remote(own_first, first.at[col], send.at[0], recv.at[0], upward),
            remote(own_second, second.at[col], send.at[1], recv.at[1], downward),
            remote(own_second, second.at[col], send.at[2], recv.at[2], upward),
            remote(own_first, first.at[col], send.at[3], recv.at[3], downward),
            remote(first.at[down], first.at[down], send.at[4], recv.at[4], upward),
            remote(second.at[up], second.at[up], send.at[5], recv.at[5], downward),
        ]

    inv_ring = ring((inverse_ref.at[0, 0], inverse_ref.at[0, 1]), inv, 0)
    cpl_ring = ring((coupling_ref.at[0, 0], coupling_ref.at[0, 1]), cpl, 1)
    own_inv = pltpu.make_async_copy(inverse_ref.at[0], inv.at[col], local_sem.at[0])
    own_cpl = pltpu.make_async_copy(coupling_ref.at[0], cpl.at[col], local_sem.at[1])
    own_src = pltpu.make_async_copy(source_ref.at[0], src, local_sem.at[2])
    own_inv.start()
    own_cpl.start()
    own_src.start()

    @pl.when(core == 0)
    def _():
        pl.semaphore_wait(turn_sem, 1)

    for copy in inv_ring[:4]:
        copy.start()

    active = (lax.broadcasted_iota(jnp.int32, (1, width), 1) < count_ref[0]).astype(jnp.float32)

    def take_inverse(which):
        rows = pl.ds(pl.multiple_of(which * block, block), block)
        for part in range(2):
            high, low = split(inv[which, part].T * active)
            inv_high[rows, part * width : (part + 1) * width] = high
            inv_low[rows, part * width : (part + 1) * width] = low

    own_inv.wait()
    take_inverse(col)
    inv_ring[0].wait_recv()
    inv_ring[4].start()
    inv_ring[1].wait_recv()
    inv_ring[5].start()
    for copy in cpl_ring[:4]:
        copy.start()
    inv_ring[2].wait_recv()
    take_inverse(down)
    inv_ring[3].wait_recv()
    take_inverse(up)
    inv_ring[4].wait_recv()
    inv_ring[5].wait_recv()
    take_inverse(across)

    def even_map_copy(which):
        return remote(
            even_map.at[which], even_in.at[which], core_send.at[which], core_recv.at[which], partner
        )

    def take_coupling(which):
        rows = pl.ds(pl.multiple_of(which * block, block), block)
        real, imag = product(cpl[which, 0].T, cpl[which, 1].T, inv_high, inv_low)
        for part, value in enumerate((real, imag)):
            high, low = split(value)
            own_high[rows, part * width : (part + 1) * width] = high
            own_low[rows, part * width : (part + 1) * width] = low

        @pl.when(core == 0)
        def _():
            even_map[which, :, :width] = real
            even_map[which, :, width:] = imag
            even_map_copy(which).start()

    own_cpl.wait()
    take_coupling(col)
    own_src.wait()
    for start in range(0, columns, block):
        real, imag = product(
            src[0, :, start : start + block].T, src[1, :, start : start + block].T, inv_high, inv_low
        )
        offset[start : start + block, :width] = real
        offset[start : start + block, width:] = imag

    even_offset_copy = remote(offset, even_offset, core_send.at[ROWS], core_recv.at[ROWS], partner)

    @pl.when(core == 0)
    def _():
        even_offset_copy.start()

    cpl_ring[0].wait_recv()
    cpl_ring[4].start()
    cpl_ring[1].wait_recv()
    cpl_ring[5].start()
    cpl_ring[2].wait_recv()
    cpl_ring[3].wait_recv()

    @pl.when(core == 1)
    def _():
        pl.semaphore_signal(turn_sem, inc=1, device_id=partner, device_id_type=MESH)

    take_coupling(down)
    take_coupling(up)
    cpl_ring[4].wait_recv()
    cpl_ring[5].wait_recv()
    take_coupling(across)
    for copy in inv_ring + cpl_ring:
        copy.wait_send()

    def rows_of(step, index):
        return pl.ds(pl.multiple_of(index * step, step), step)

    def chunk(ref, rows):
        return ref[rows, :width], ref[rows, width:]

    def put(ref, rows, value):
        ref[rows, :width] = value[0]
        ref[rows, width:] = value[1]

    def plus(value, other):
        return value[0] + other[0], value[1] + other[1]

    next_odd = at(z, x_next, 1)

    def map_copy(index):
        rows = rows_of(map_step, index)
        return remote(
            map_out.at[rows], map_in.at[rows], map_send.at[index], map_recv.at[index], next_odd
        )

    def off_copy(index):
        rows = rows_of(off_step, index)
        return remote(
            off_out.at[rows], off_in.at[rows], off_send.at[index], off_recv.at[index], next_odd
        )

    maps = map_recv.shape[0]

    def whole_copy(kind, index):
        rows = rows_of(map_step, index)
        send, recv = whole_send.at[kind, index], whole_recv.at[kind, index]
        if kind < 2:
            return remote(map_out.at[rows], whole.at[col, rows], send, recv, (upward, downward)[kind])
        if index < maps // 2:
            return remote(whole.at[down, rows], whole.at[down, rows], send, recv, upward)
        return remote(whole.at[up, rows], whole.at[up, rows], send, recv, downward)

    def forward(index):
        whole_copy(0 if index < maps // 2 else 1, index).wait_recv()
        whole_copy(2, index).start()

    ends = off_recv.shape[0]
    early = ends // 2

    def first_copy(index):
        rows = rows_of(off_step, index)
        return remote(
            off_out.at[rows], z_in.at[rows], out_send.at[index], z_recv.at[index], at(1, 3, 1)
        )

    def offsets(index, count):
        rows = pl.ds(pl.multiple_of(index * off_step, off_step), count * off_step)
        for extra in range(count):
            off_copy(index + extra).wait_recv()
        value = product(*chunk(off_in, rows), pair_high, pair_low)
        put(off_out, rows, plus(value, chunk(offset, rows)))
        for extra in range(count):

            @pl.when(x < 3)
            def _():
                off_copy(index + extra).start()

            @pl.when((x == 3) & (z == 0))
            def _():
                first_copy(index + extra).start()

    @pl.when(core == 1)
    def _():
        def compose(which):
            rows = pl.ds(pl.multiple_of(which * block, block), block)
            even_map_copy(which).wait_recv()
            value = product(even_in[which, :, :width], even_in[which, :, width:], own_high, own_low)
            for part in range(2):
                high, low = split(value[part])
                pair_high[rows, part * width : (part + 1) * width] = high
                pair_low[rows, part * width : (part + 1) * width] = low
            return value

        first = compose(col)

        @pl.when(x == 0)
        def _():
            put(map_out, slice(None), first)
            for index in range(map_recv.shape[0]):
                map_copy(index).start()

        even_offset_copy.wait_recv()

        def compose_offset(index, carry):
            rows = rows_of(block, index)
            value = product(*chunk(even_offset, rows), own_high, own_low)
            put(offset, rows, plus(value, chunk(offset, rows)))
            return carry

        lax.fori_loop(0, columns // block, compose_offset, 0)

        @pl.when(x == 0)
        def _():
            off_out[...] = offset[...]
            for index in range(off_recv.shape[0]):
                off_copy(index).start()

        for which in (down, up, across):
            compose(which)

        @pl.when(x > 0)
        def _():
            def map_sweep(index, carry):
                rows = rows_of(map_step, index)
                map_copy(index).wait_recv()
                put(map_out, rows, product(*chunk(map_in, rows), pair_high, pair_low))

                @pl.when(x < 3)
                def _():
                    map_copy(index).start()

                @pl.when(x == 3)
                def _():
                    whole_copy(0, index).start()
                    whole_copy(1, index).start()

                return carry

            lax.fori_loop(0, map_recv.shape[0], map_sweep, 0)

            def off_sweep(index, carry):
                offsets(index, 1)
                return carry

            done = 0
            for index in range(maps):
                until = max(0, index - maps // 2)
                if until > done:
                    lax.fori_loop(done, until, off_sweep, 0)
                    done = until

                @pl.when(x == 3)
                def _():
                    forward(index)

            lax.fori_loop(done, early, off_sweep, 0)

            @pl.when((x < 3) | (z == 0))
            def _():
                lax.fori_loop(early, ends, off_sweep, 0)

        @pl.when(x < 3)
        def _():
            for index in range(maps):
                whole_copy(0, index).start()
                whole_copy(1, index).start()
            for index in range(maps):
                forward(index)
            for index in range(map_recv.shape[0]):
                map_copy(index).wait_send()
            for index in range(off_recv.shape[0]):
                off_copy(index).wait_send()

        def take_whole(which):
            rows = pl.ds(pl.multiple_of(which * block, block), block)
            high, low = split(whole[which])
            whole_high[rows] = high
            whole_low[rows] = low

        whole[col] = map_out[...]
        take_whole(col)
        for index in range(maps // 2, maps):
            whole_copy(0, index).wait_recv()
        take_whole(down)
        for index in range(maps // 2):
            whole_copy(1, index).wait_recv()
        take_whole(up)
        for index in range(maps):
            whole_copy(2, index).wait_recv()
        take_whole(across)
        for kind in range(3):
            for index in range(maps):
                whole_copy(kind, index).wait_send()

    def z_copy(index):
        rows = rows_of(end_step, index)
        return remote(
            state.at[rows], z_in.at[rows], out_send.at[index], z_recv.at[index], at((z + 1) % planes, 3, 1)
        )

    def enter_copy(index):
        rows = rows_of(end_step, index)
        return remote(
            z_in.at[rows], x_in.at[rows], pass_send.at[index], x_recv.at[index], at(z, 0, 1)
        )

    def enter_back_copy(index):
        rows = rows_of(end_step, index)
        return remote(
            z_in.at[rows], x_in.at[rows], back_send.at[index], x_recv.at[index], at(z, 2, 1)
        )

    def back_copy(index):
        rows = rows_of(end_step, index)
        return remote(
            x_in.at[rows], x_in.at[rows], back_send.at[index], x_recv.at[index], at(z, x_before, 1)
        )

    def pass_copy(index):
        rows = rows_of(end_step, index)
        return remote(
            x_in.at[rows], x_in.at[rows], pass_send.at[index], x_recv.at[index], partner
        )

    def x_copy(index):
        rows = rows_of(end_step, index)
        return remote(
            state.at[rows], x_in.at[rows], out_send.at[index], x_recv.at[index], at(z, x_next, 0)
        )

    @pl.when((core == 1) & (x == 3))
    def _():
        @pl.when(z == 0)
        def _():
            z_in[...] = jnp.zeros_like(z_in)
            state[...] = off_out[...]
            for index in range(ends):
                enter_copy(index).start()
                enter_back_copy(index).start()

        @pl.when(z > 0)
        def _():
            def z_sweep(index, carry):
                rows = rows_of(end_step, index)
                z_copy(index).wait_recv()
                enter_copy(index).start()
                enter_back_copy(index).start()
                value = product(*chunk(z_in, rows), whole_high, whole_low)
                put(state, rows, plus(value, chunk(off_out, rows)))

                @pl.when(z < planes - 1)
                def _():
                    z_copy(index).start()

                return carry

            def both_sweep(index, carry):
                offsets(early + 2 * index, 2)
                z_sweep(2 * index, carry)
                return z_sweep(2 * index + 1, carry)

            lax.fori_loop(0, (ends - early) // 2, both_sweep, 0)
            lax.fori_loop(ends - early, ends, z_sweep, 0)

        @pl.when(z < planes - 1)
        def _():
            for index in range(ends):
                z_copy(index).wait_send()

        for index in range(ends):
            enter_copy(index).wait_send()
            enter_back_copy(index).wait_send()

    @pl.when((core == 1) & (x < 3))
    def _():
        def x_sweep(index, carry):
            rows = rows_of(end_step, index)
            x_copy(index).wait_recv()

            @pl.when(x == 2)
            def _():
                back_copy(index).start()

            @pl.when(x == 0)
            def _():
                pass_copy(index).start()

            value = product(*chunk(x_in, rows), whole_high, whole_low)
            put(state, rows, plus(value, chunk(off_out, rows)))
            x_copy(index).start()
            return carry

        lax.fori_loop(0, ends, x_sweep, 0)
        for index in range(ends):
            x_copy(index).wait_send()

        @pl.when(x == 2)
        def _():
            for index in range(ends):
                back_copy(index).wait_send()

        @pl.when(x == 0)
        def _():
            for index in range(ends):
                pass_copy(index).wait_send()

    @pl.when(core == 0)
    def _():
        def even_sweep(index, carry):
            rows = rows_of(end_step, index)
            x_copy(index).wait_recv()
            value = product(*chunk(x_in, rows), own_high, own_low)
            put(state, rows, plus(value, chunk(offset, rows)))
            return carry

        lax.fori_loop(0, ends, even_sweep, 0)
        for which in range(ROWS):
            even_map_copy(which).wait_send()
        even_offset_copy.wait_send()

    for start in range(0, columns, block):
        for part in range(2):
            out_ref[0, part, :, start : start + block] = state[
                start : start + block, part * width : (part + 1) * width
            ].T


def local(planes, inverses, couplings, sources, counts):
    width, block = inverses.shape[2], inverses.shape[3]
    columns = sources.shape[3]
    map_chunks, end_chunks = 8, 16
    single, half = jnp.float32, jnp.bfloat16
    vmem, dma = pltpu.VMEM, pltpu.SemaphoreType.DMA
    held_map = vmem((width, 2 * width), half)
    rows_buffer = vmem((columns, 2 * width), single)
    map_buffer = vmem((block, 2 * width), single)
    any_space = pl.BlockSpec(memory_space=pl.ANY)
    in_vmem = pl.BlockSpec(memory_space=pltpu.VMEM)
    return pl.pallas_call(
        functools.partial(kernel, planes),
        out_shape=jax.ShapeDtypeStruct(sources.shape, single),
        in_specs=[any_space, any_space, any_space, pl.BlockSpec(memory_space=pltpu.SMEM)],
        out_specs=in_vmem,
        scratch_shapes=[
            vmem((ROWS, 2, width, block), single),
            vmem((ROWS, 2, width, block), single),
            vmem((2, width, columns), single),
            held_map,
            held_map,
            held_map,
            held_map,
            held_map,
            held_map,
            vmem((ROWS, block, 2 * width), single),
            vmem((ROWS, block, 2 * width), single),
            rows_buffer,
            rows_buffer,
            map_buffer,
            map_buffer,
            rows_buffer,
            rows_buffer,
            vmem((ROWS, block, 2 * width), single),
            held_map,
            held_map,
            rows_buffer,
            rows_buffer,
            rows_buffer,
            dma((3,)),
            dma((2, 6)),
            dma((2, 6)),
            dma((ROWS + 1,)),
            dma((ROWS + 1,)),
            dma((map_chunks,)),
            dma((map_chunks,)),
            dma((end_chunks,)),
            dma((end_chunks,)),
            dma((end_chunks,)),
            dma((end_chunks,)),
            dma((end_chunks,)),
            dma((end_chunks,)),
            dma((end_chunks,)),
            dma((3, map_chunks)),
            dma((3, map_chunks)),
            pltpu.SemaphoreType.REGULAR,
        ],
        compiler_params=pltpu.CompilerParams(
            collective_id=0, has_side_effects=True, vmem_limit_bytes=40 * 2**20
        ),
    )(inverses, couplings, sources, counts)


def solution(mesh):
    placed = (
        P("chain", None, None, "col"),
        P("chain", None, None, "col"),
        P("chain", None, None, "col"),
        P("chain"),
    )
    return jax.shard_map(
        functools.partial(local, mesh.shape["chain"] // PLANE),
        mesh=mesh,
        in_specs=placed,
        out_specs=P("chain", None, None, "col"),
        check_vma=False,
    )
```

```python
import functools

import jax
import jax.numpy as jnp
from jax import lax
from jax.experimental import pallas as pl
from jax.experimental.pallas import tpu as pltpu
from jax.sharding import PartitionSpec as P

MESH = pl.DeviceIdType.MESH
PLANE = 8
ROWS = 4


def split(value):
    high = value.astype(jnp.bfloat16)
    return high, (value - high.astype(jnp.float32)).astype(jnp.bfloat16)


def product(real, imag, high_ref, low_ref):
    count, width = real.shape
    tile = min(256, width)
    real_high, real_low = split(real)
    imag_high, imag_low = split(imag)
    high = jnp.concatenate([real_high, imag_high], axis=0)
    both = jnp.concatenate([real_high, imag_high, real_low, imag_low], axis=0)

    def against(columns):
        wide = jnp.dot(both, high_ref[:, columns], preferred_element_type=jnp.float32)
        narrow = jnp.dot(high, low_ref[:, columns], preferred_element_type=jnp.float32)
        return wide[: 2 * count] + (wide[2 * count :] + narrow)

    reals, imags = [], []
    for start in range(0, width, tile):
        by_real = against(slice(start, start + tile))
        by_imag = against(slice(width + start, width + start + tile))
        reals.append(by_real[:count] - by_imag[count:])
        imags.append(by_imag[:count] + by_real[count:])
    return jnp.concatenate(reals, axis=1), jnp.concatenate(imags, axis=1)


def kernel(
    planes,
    inverse_ref,
    coupling_ref,
    source_ref,
    count_ref,
    out_ref,
    inv,
    cpl,
    src,
    inv_high,
    inv_low,
    own_high,
    own_low,
    pair_high,
    pair_low,
    even_map,
    even_in,
    even_offset,
    offset,
    map_in,
    map_out,
    off_in,
    off_out,
    whole,
    whole_high,
    whole_low,
    z_in,
    x_in,
    state,
    local_sem,
    gather_send,
    gather_recv,
    core_send,
    core_recv,
    map_send,
    map_recv,
    off_send,
    off_recv,
    z_recv,
    x_recv,
    out_send,
    pass_send,
    back_send,
    whole_send,
    whole_recv,
    turn_sem,
):
    width = inv_high.shape[0]
    block = width // ROWS
    columns = offset.shape[0]
    map_step = block // map_recv.shape[0]
    off_step = columns // off_recv.shape[0]
    end_step = columns // z_recv.shape[0]

    place = lax.axis_index("chain")
    col = lax.axis_index("col")
    z = place // PLANE
    x = (place % PLANE) // 2
    core = place % 2
    up, down, across = (col + 1) % ROWS, (col + 3) % ROWS, (col + 2) % ROWS

    def at(z_to, x_to, core_to):
        return {"chain": z_to * PLANE + x_to * 2 + core_to, "col": col}

    partner = at(z, x, 1 - core)
    upward = {"chain": place, "col": up}
    downward = {"chain": place, "col": down}
    x_next, x_before = (x + 1) % 4, (x + 3) % 4
    odd, last = core == 1, (core == 1) & (x == 3)

    own_inv = pltpu.make_async_copy(inverse_ref.at[0], inv.at[col], local_sem.at[0])
    own_cpl = pltpu.make_async_copy(coupling_ref.at[0], cpl.at[col], local_sem.at[1])
    own_src = pltpu.make_async_copy(source_ref.at[0], src, local_sem.at[2])
    own_inv.start()
    own_cpl.start()
    own_src.start()

    barrier = pltpu.get_barrier_semaphore()

    def greet(when, device):
        @pl.when(when)
        def _():
            pl.semaphore_signal(barrier, inc=1, device_id=device, device_id_type=MESH)

        return jnp.where(when, 1, 0)

    for device in (upward, downward, partner):
        pl.semaphore_signal(barrier, inc=1, device_id=device, device_id_type=MESH)
    greeted = 3
    greeted += greet(odd, at(z, x_next, 1))
    greeted += greet(odd, at(z, x_before, 1))
    greeted += greet(odd & (x < 3), at(z, x_next, 0))
    greeted += greet((core == 0) & (x > 0), at(z, x_before, 1))
    greeted += greet(last & (z < planes - 1), at(z + 1, 3, 1))
    greeted += greet(last & (z > 0), at(z - 1, 3, 1))
    pl.semaphore_wait(barrier, greeted)

    def remote(source, target, send, recv, device):
        return pltpu.make_async_remote_copy(
            src_ref=source,
            dst_ref=target,
            send_sem=send,
            recv_sem=recv,
            device_id=device,
            device_id_type=MESH,
        )

    def ring(held, which):
        send, recv = gather_send.at[which], gather_recv.at[which]
        first, second = held.at[:, 0], held.at[:, 1]
        own_first, own_second = first.at[col], second.at[col]
        return [
            remote(own_first, first.at[col], send.at[0], recv.at[0], upward),
            remote(own_second, second.at[col], send.at[1], recv.at[1], downward),
            remote(own_second, second.at[col], send.at[2], recv.at[2], upward),
            remote(own_first, first.at[col], send.at[3], recv.at[3], downward),
            remote(first.at[down], first.at[down], send.at[4], recv.at[4], upward),
            remote(second.at[up], second.at[up], send.at[5], recv.at[5], downward),
        ]

    inv_ring = ring(inv, 0)
    cpl_ring = ring(cpl, 1)
    @pl.when(core == 0)
    def _():
        pl.semaphore_wait(turn_sem, 1)

    own_inv.wait()
    for copy in inv_ring[:4]:
        copy.start()

    active = (lax.broadcasted_iota(jnp.int32, (1, width), 1) < count_ref[0]).astype(jnp.float32)

    def take_inverse(which):
        rows = pl.ds(pl.multiple_of(which * block, block), block)
        for part in range(2):
            high, low = split(inv[which, part].T * active)
            inv_high[rows, part * width : (part + 1) * width] = high
            inv_low[rows, part * width : (part + 1) * width] = low

    take_inverse(col)
    inv_ring[0].wait_recv()
    inv_ring[4].start()
    inv_ring[1].wait_recv()
    inv_ring[5].start()
    own_cpl.wait()
    for copy in cpl_ring[:4]:
        copy.start()
    inv_ring[2].wait_recv()
    take_inverse(down)
    inv_ring[3].wait_recv()
    take_inverse(up)
    inv_ring[4].wait_recv()
    inv_ring[5].wait_recv()
    take_inverse(across)

    def even_map_copy(which):
        return remote(
            even_map.at[which], even_in.at[which], core_send.at[which], core_recv.at[which], partner
        )

    def take_coupling(which):
        rows = pl.ds(pl.multiple_of(which * block, block), block)
        real, imag = product(cpl[which, 0].T, cpl[which, 1].T, inv_high, inv_low)
        for part, value in enumerate((real, imag)):
            high, low = split(value)
            own_high[rows, part * width : (part + 1) * width] = high
            own_low[rows, part * width : (part + 1) * width] = low

        @pl.when(core == 0)
        def _():
            even_map[which, :, :width] = real
            even_map[which, :, width:] = imag
            even_map_copy(which).start()

    take_coupling(col)
    own_src.wait()
    for start in range(0, columns, block):
        real, imag = product(
            src[0, :, start : start + block].T, src[1, :, start : start + block].T, inv_high, inv_low
        )
        offset[start : start + block, :width] = real
        offset[start : start + block, width:] = imag

    even_offset_copy = remote(offset, even_offset, core_send.at[ROWS], core_recv.at[ROWS], partner)

    @pl.when(core == 0)
    def _():
        even_offset_copy.start()

    cpl_ring[0].wait_recv()
    cpl_ring[4].start()
    cpl_ring[1].wait_recv()
    cpl_ring[5].start()
    cpl_ring[2].wait_recv()
    cpl_ring[3].wait_recv()

    @pl.when(core == 1)
    def _():
        pl.semaphore_signal(turn_sem, inc=1, device_id=partner, device_id_type=MESH)

    take_coupling(down)
    take_coupling(up)
    cpl_ring[4].wait_recv()
    cpl_ring[5].wait_recv()
    take_coupling(across)
    for copy in inv_ring + cpl_ring:
        copy.wait_send()

    def rows_of(step, index):
        return pl.ds(pl.multiple_of(index * step, step), step)

    def chunk(ref, rows):
        return ref[rows, :width], ref[rows, width:]

    def put(ref, rows, value):
        ref[rows, :width] = value[0]
        ref[rows, width:] = value[1]

    def plus(value, other):
        return value[0] + other[0], value[1] + other[1]

    next_odd = at(z, x_next, 1)

    def map_copy(index):
        rows = rows_of(map_step, index)
        return remote(
            map_out.at[rows], map_in.at[rows], map_send.at[index], map_recv.at[index], next_odd
        )

    def off_copy(index):
        rows = rows_of(off_step, index)
        return remote(
            off_out.at[rows], off_in.at[rows], off_send.at[index], off_recv.at[index], next_odd
        )

    maps = map_recv.shape[0]

    def whole_copy(kind, index):
        rows = rows_of(map_step, index)
        send, recv = whole_send.at[kind, index], whole_recv.at[kind, index]
        if kind < 2:
            return remote(map_out.at[rows], whole.at[col, rows], send, recv, (upward, downward)[kind])
        if index < maps // 2:
            return remote(whole.at[down, rows], whole.at[down, rows], send, recv, upward)
        return remote(whole.at[up, rows], whole.at[up, rows], send, recv, downward)

    def forward(index):
        whole_copy(0 if index < maps // 2 else 1, index).wait_recv()
        whole_copy(2, index).start()

    ends = off_recv.shape[0]
    early = ends // 2

    def first_copy(index):
        rows = rows_of(off_step, index)
        return remote(
            off_out.at[rows], z_in.at[rows], out_send.at[index], z_recv.at[index], at(1, 3, 1)
        )

    def offsets(index, count):
        rows = pl.ds(pl.multiple_of(index * off_step, off_step), count * off_step)
        for extra in range(count):
            off_copy(index + extra).wait_recv()
        value = product(*chunk(off_in, rows), pair_high, pair_low)
        put(off_out, rows, plus(value, chunk(offset, rows)))
        for extra in range(count):

            @pl.when(x < 3)
            def _():
                off_copy(index + extra).start()

            @pl.when((x == 3) & (z == 0))
            def _():
                first_copy(index + extra).start()

    @pl.when(core == 1)
    def _():
        def compose(which):
            rows = pl.ds(pl.multiple_of(which * block, block), block)
            even_map_copy(which).wait_recv()
            value = product(even_in[which, :, :width], even_in[which, :, width:], own_high, own_low)
            for part in range(2):
                high, low = split(value[part])
                pair_high[rows, part * width : (part + 1) * width] = high
                pair_low[rows, part * width : (part + 1) * width] = low
            return value

        first = compose(col)

        @pl.when(x == 0)
        def _():
            put(map_out, slice(None), first)
            for index in range(map_recv.shape[0]):
                map_copy(index).start()

        even_offset_copy.wait_recv()

        def compose_offset(index, carry):
            rows = rows_of(block, index)
            value = product(*chunk(even_offset, rows), own_high, own_low)
            put(offset, rows, plus(value, chunk(offset, rows)))
            return carry

        lax.fori_loop(0, columns // block, compose_offset, 0)

        @pl.when(x == 0)
        def _():
            off_out[...] = offset[...]
            for index in range(off_recv.shape[0]):
                off_copy(index).start()

        for which in (down, up, across):
            compose(which)

        @pl.when(x == 0)
        def _():
            for index in range(maps):
                whole_copy(0, index).start()
                whole_copy(1, index).start()
            for index in range(maps):
                forward(index)

        @pl.when(x > 0)
        def _():
            def map_sweep(index, carry):
                rows = rows_of(map_step, index)
                map_copy(index).wait_recv()
                put(map_out, rows, product(*chunk(map_in, rows), pair_high, pair_low))

                @pl.when(x < 3)
                def _():
                    map_copy(index).start()

                whole_copy(0, index).start()
                whole_copy(1, index).start()

                return carry

            lax.fori_loop(0, map_recv.shape[0], map_sweep, 0)

            def off_sweep(index, carry):
                offsets(index, 1)
                return carry

            done = 0
            for index in range(maps):
                until = max(0, index - maps // 2)
                if until > done:
                    lax.fori_loop(done, until, off_sweep, 0)
                    done = until
                forward(index)

            lax.fori_loop(done, early, off_sweep, 0)

            @pl.when((x < 3) | (z == 0))
            def _():
                lax.fori_loop(early, ends, off_sweep, 0)

        @pl.when(x < 3)
        def _():
            for index in range(map_recv.shape[0]):
                map_copy(index).wait_send()
            for index in range(off_recv.shape[0]):
                off_copy(index).wait_send()

        def take_whole(which):
            rows = pl.ds(pl.multiple_of(which * block, block), block)
            high, low = split(whole[which])
            whole_high[rows] = high
            whole_low[rows] = low

        whole[col] = map_out[...]
        take_whole(col)
        for index in range(maps // 2, maps):
            whole_copy(0, index).wait_recv()
        take_whole(down)
        for index in range(maps // 2):
            whole_copy(1, index).wait_recv()
        take_whole(up)
        for index in range(maps):
            whole_copy(2, index).wait_recv()
        take_whole(across)
        for kind in range(3):
            for index in range(maps):
                whole_copy(kind, index).wait_send()

    def z_copy(index):
        rows = rows_of(end_step, index)
        return remote(
            state.at[rows], z_in.at[rows], out_send.at[index], z_recv.at[index], at((z + 1) % planes, 3, 1)
        )

    def enter_copy(index):
        rows = rows_of(end_step, index)
        return remote(
            z_in.at[rows], x_in.at[rows], pass_send.at[index], x_recv.at[index], at(z, 0, 1)
        )

    def enter_back_copy(index):
        rows = rows_of(end_step, index)
        return remote(
            z_in.at[rows], x_in.at[rows], back_send.at[index], x_recv.at[index], at(z, 2, 1)
        )

    def back_copy(index):
        rows = rows_of(end_step, index)
        return remote(
            x_in.at[rows], x_in.at[rows], back_send.at[index], x_recv.at[index], at(z, x_before, 1)
        )

    def pass_copy(index):
        rows = rows_of(end_step, index)
        return remote(
            x_in.at[rows], x_in.at[rows], pass_send.at[index], x_recv.at[index], partner
        )

    def x_copy(index):
        rows = rows_of(end_step, index)
        return remote(
            state.at[rows], x_in.at[rows], out_send.at[index], x_recv.at[index], at(z, x_next, 0)
        )

    @pl.when((core == 1) & (x == 3))
    def _():
        @pl.when(z == 0)
        def _():
            z_in[...] = jnp.zeros_like(z_in)
            state[...] = off_out[...]
            for index in range(ends):
                enter_copy(index).start()
                enter_back_copy(index).start()

        @pl.when(z > 0)
        def _():
            def z_sweep(index, carry):
                rows = rows_of(end_step, index)
                z_copy(index).wait_recv()
                enter_copy(index).start()
                enter_back_copy(index).start()
                value = product(*chunk(z_in, rows), whole_high, whole_low)
                put(state, rows, plus(value, chunk(off_out, rows)))

                @pl.when(z < planes - 1)
                def _():
                    z_copy(index).start()

                return carry

            def both_sweep(index, carry):
                offsets(early + 2 * index, 2)
                z_sweep(2 * index, carry)
                return z_sweep(2 * index + 1, carry)

            lax.fori_loop(0, (ends - early) // 2, both_sweep, 0)
            lax.fori_loop(ends - early, ends, z_sweep, 0)

        @pl.when(z < planes - 1)
        def _():
            for index in range(ends):
                z_copy(index).wait_send()

        for index in range(ends):
            enter_copy(index).wait_send()
            enter_back_copy(index).wait_send()

    @pl.when((core == 1) & (x < 3))
    def _():
        def x_sweep(index, carry):
            rows = rows_of(end_step, index)
            x_copy(index).wait_recv()

            @pl.when(x == 2)
            def _():
                back_copy(index).start()

            @pl.when(x == 0)
            def _():
                pass_copy(index).start()

            value = product(*chunk(x_in, rows), whole_high, whole_low)
            put(state, rows, plus(value, chunk(off_out, rows)))
            x_copy(index).start()
            return carry

        lax.fori_loop(0, ends, x_sweep, 0)
        for index in range(ends):
            x_copy(index).wait_send()

        @pl.when(x == 2)
        def _():
            for index in range(ends):
                back_copy(index).wait_send()

        @pl.when(x == 0)
        def _():
            for index in range(ends):
                pass_copy(index).wait_send()

    @pl.when(core == 0)
    def _():
        def even_sweep(index, carry):
            rows = rows_of(end_step, index)
            x_copy(index).wait_recv()
            value = product(*chunk(x_in, rows), own_high, own_low)
            put(state, rows, plus(value, chunk(offset, rows)))
            return carry

        lax.fori_loop(0, ends, even_sweep, 0)
        for which in range(ROWS):
            even_map_copy(which).wait_send()
        even_offset_copy.wait_send()

    for start in range(0, columns, block):
        for part in range(2):
            out_ref[0, part, :, start : start + block] = state[
                start : start + block, part * width : (part + 1) * width
            ].T


def local(planes, inverses, couplings, sources, counts):
    width, block = inverses.shape[2], inverses.shape[3]
    columns = sources.shape[3]
    map_chunks, end_chunks = 8, 16
    single, half = jnp.float32, jnp.bfloat16
    vmem, dma = pltpu.VMEM, pltpu.SemaphoreType.DMA
    held_map = vmem((width, 2 * width), half)
    rows_buffer = vmem((columns, 2 * width), single)
    map_buffer = vmem((block, 2 * width), single)
    in_hbm = pl.BlockSpec(memory_space=pltpu.HBM)
    in_vmem = pl.BlockSpec(memory_space=pltpu.VMEM)
    return pl.pallas_call(
        functools.partial(kernel, planes),
        out_shape=jax.ShapeDtypeStruct(sources.shape, single),
        in_specs=[in_hbm, in_hbm, in_hbm, pl.BlockSpec(memory_space=pltpu.SMEM)],
        out_specs=in_vmem,
        scratch_shapes=[
            vmem((ROWS, 2, width, block), single),
            vmem((ROWS, 2, width, block), single),
            vmem((2, width, columns), single),
            held_map,
            held_map,
            held_map,
            held_map,
            held_map,
            held_map,
            vmem((ROWS, block, 2 * width), single),
            vmem((ROWS, block, 2 * width), single),
            rows_buffer,
            rows_buffer,
            map_buffer,
            map_buffer,
            rows_buffer,
            rows_buffer,
            vmem((ROWS, block, 2 * width), single),
            held_map,
            held_map,
            rows_buffer,
            rows_buffer,
            rows_buffer,
            dma((3,)),
            dma((2, 6)),
            dma((2, 6)),
            dma((ROWS + 1,)),
            dma((ROWS + 1,)),
            dma((map_chunks,)),
            dma((map_chunks,)),
            dma((end_chunks,)),
            dma((end_chunks,)),
            dma((end_chunks,)),
            dma((end_chunks,)),
            dma((end_chunks,)),
            dma((end_chunks,)),
            dma((end_chunks,)),
            dma((3, map_chunks)),
            dma((3, map_chunks)),
            pltpu.SemaphoreType.REGULAR,
        ],
        compiler_params=pltpu.CompilerParams(
            collective_id=0, has_side_effects=True, vmem_limit_bytes=40 * 2**20
        ),
    )(*(pltpu.with_memory_space_constraint(v, pltpu.HBM) for v in (inverses, couplings, sources)), counts)


def solution(mesh):
    placed = (
        P("chain", None, None, "col"),
        P("chain", None, None, "col"),
        P("chain", None, None, "col"),
        P("chain"),
    )
    return jax.shard_map(
        functools.partial(local, mesh.shape["chain"] // PLANE),
        mesh=mesh,
        in_specs=placed,
        out_specs=P("chain", None, None, "col"),
        check_vma=False,
    )
```

```python
import functools

import jax
import jax.numpy as jnp
from jax import lax
from jax.experimental import pallas as pl
from jax.experimental.pallas import tpu as pltpu
from jax.sharding import PartitionSpec as P

MESH = pl.DeviceIdType.MESH
PLANE = 8
ROWS = 4


def split(value):
    high = value.astype(jnp.bfloat16)
    return high, (value - high.astype(jnp.float32)).astype(jnp.bfloat16)


def product(real, imag, high_ref, low_ref):
    count, width = real.shape
    tile = min(256, width)
    real_high, real_low = split(real)
    imag_high, imag_low = split(imag)
    high = jnp.concatenate([real_high, imag_high], axis=0)
    both = jnp.concatenate([real_high, imag_high, real_low, imag_low], axis=0)

    def against(columns):
        wide = jnp.dot(both, high_ref[:, columns], preferred_element_type=jnp.float32)
        narrow = jnp.dot(high, low_ref[:, columns], preferred_element_type=jnp.float32)
        return wide[: 2 * count] + (wide[2 * count :] + narrow)

    reals, imags = [], []
    for start in range(0, width, tile):
        by_real = against(slice(start, start + tile))
        by_imag = against(slice(width + start, width + start + tile))
        reals.append(by_real[:count] - by_imag[count:])
        imags.append(by_imag[:count] + by_real[count:])
    return jnp.concatenate(reals, axis=1), jnp.concatenate(imags, axis=1)


def kernel(
    planes,
    inverse_ref,
    coupling_ref,
    source_ref,
    count_ref,
    out_ref,
    inv,
    cpl,
    src,
    inv_high,
    inv_low,
    own_high,
    own_low,
    pair_high,
    pair_low,
    even_map,
    even_in,
    even_offset,
    offset,
    map_in,
    map_out,
    off_in,
    off_out,
    whole,
    whole_high,
    whole_low,
    z_in,
    x_in,
    state,
    local_sem,
    gather_send,
    gather_recv,
    core_send,
    core_recv,
    map_send,
    map_recv,
    off_send,
    off_recv,
    z_recv,
    x_recv,
    out_send,
    pass_send,
    back_send,
    whole_send,
    whole_recv,
    core_pass,
    turn_sem,
):
    width = inv_high.shape[0]
    block = width // ROWS
    columns = offset.shape[0]
    map_step = block // map_recv.shape[0]
    off_step = columns // off_recv.shape[0]
    end_step = columns // z_recv.shape[0]

    place = lax.axis_index("chain")
    col = lax.axis_index("col")
    z = place // PLANE
    x = (place % PLANE) // 2
    core = place % 2
    up, down, across = (col + 1) % ROWS, (col + 3) % ROWS, (col + 2) % ROWS

    def at(z_to, x_to, core_to):
        return {"chain": z_to * PLANE + x_to * 2 + core_to, "col": col}

    partner = at(z, x, 1 - core)
    upward = {"chain": place, "col": up}
    downward = {"chain": place, "col": down}
    x_next, x_before = (x + 1) % 4, (x + 3) % 4
    odd, last = core == 1, (core == 1) & (x == 3)

    own_inv = pltpu.make_async_copy(inverse_ref.at[0], inv.at[col], local_sem.at[0])
    own_cpl = pltpu.make_async_copy(coupling_ref.at[0], cpl.at[col], local_sem.at[1])
    own_src = pltpu.make_async_copy(source_ref.at[0], src, local_sem.at[2])
    own_inv.start()
    own_cpl.start()
    own_src.start()

    barrier = pltpu.get_barrier_semaphore()

    def greet(when, device):
        @pl.when(when)
        def _():
            pl.semaphore_signal(barrier, inc=1, device_id=device, device_id_type=MESH)

        return jnp.where(when, 1, 0)

    for device in (upward, downward, partner):
        pl.semaphore_signal(barrier, inc=1, device_id=device, device_id_type=MESH)
    greeted = 3
    greeted += greet(odd, at(z, x_next, 1))
    greeted += greet(odd, at(z, x_before, 1))
    greeted += greet(last & (z < planes - 1), at(z + 1, 3, 1))
    greeted += greet(last & (z > 0), at(z - 1, 3, 1))
    pl.semaphore_wait(barrier, greeted)

    def remote(source, target, send, recv, device):
        return pltpu.make_async_remote_copy(
            src_ref=source,
            dst_ref=target,
            send_sem=send,
            recv_sem=recv,
            device_id=device,
            device_id_type=MESH,
        )

    def ring(held, which):
        send, recv = gather_send.at[which], gather_recv.at[which]
        first, second = held.at[:, 0], held.at[:, 1]
        own_first, own_second = first.at[col], second.at[col]
        return [
            remote(own_first, first.at[col], send.at[0], recv.at[0], upward),
            remote(own_second, second.at[col], send.at[1], recv.at[1], downward),
            remote(own_second, second.at[col], send.at[2], recv.at[2], upward),
            remote(own_first, first.at[col], send.at[3], recv.at[3], downward),
            remote(first.at[down], first.at[down], send.at[4], recv.at[4], upward),
            remote(second.at[up], second.at[up], send.at[5], recv.at[5], downward),
        ]

    inv_ring = ring(inv, 0)
    cpl_ring = ring(cpl, 1)
    @pl.when(core == 0)
    def _():
        pl.semaphore_wait(turn_sem, 1)

    own_inv.wait()
    for copy in inv_ring[:4]:
        copy.start()

    active = (lax.broadcasted_iota(jnp.int32, (1, width), 1) < count_ref[0]).astype(jnp.float32)

    def take_inverse(which):
        rows = pl.ds(pl.multiple_of(which * block, block), block)
        for part in range(2):
            high, low = split(inv[which, part].T * active)
            inv_high[rows, part * width : (part + 1) * width] = high
            inv_low[rows, part * width : (part + 1) * width] = low

    take_inverse(col)
    inv_ring[0].wait_recv()
    inv_ring[4].start()
    inv_ring[1].wait_recv()
    inv_ring[5].start()
    own_cpl.wait()
    for copy in cpl_ring[:4]:
        copy.start()

    @pl.when(core == 1)
    def _():
        pl.semaphore_signal(turn_sem, inc=1, device_id=partner, device_id_type=MESH)

    inv_ring[2].wait_recv()
    take_inverse(down)
    inv_ring[3].wait_recv()
    take_inverse(up)
    inv_ring[4].wait_recv()
    inv_ring[5].wait_recv()
    take_inverse(across)

    def even_map_copy(which):
        return remote(
            even_map.at[which], even_in.at[which], core_send.at[which], core_recv.at[which], partner
        )

    def take_coupling(which):
        rows = pl.ds(pl.multiple_of(which * block, block), block)
        real, imag = product(cpl[which, 0].T, cpl[which, 1].T, inv_high, inv_low)
        for part, value in enumerate((real, imag)):
            high, low = split(value)
            own_high[rows, part * width : (part + 1) * width] = high
            own_low[rows, part * width : (part + 1) * width] = low

        @pl.when(core == 0)
        def _():
            even_map[which, :, :width] = real
            even_map[which, :, width:] = imag
            even_map_copy(which).start()

    take_coupling(col)
    own_src.wait()
    for start in range(0, columns, block):
        real, imag = product(
            src[0, :, start : start + block].T, src[1, :, start : start + block].T, inv_high, inv_low
        )
        offset[start : start + block, :width] = real
        offset[start : start + block, width:] = imag

    even_offset_copy = remote(offset, even_offset, core_send.at[ROWS], core_recv.at[ROWS], partner)

    @pl.when(core == 0)
    def _():
        even_offset_copy.start()

    cpl_ring[0].wait_recv()
    cpl_ring[4].start()
    cpl_ring[1].wait_recv()
    cpl_ring[5].start()
    cpl_ring[2].wait_recv()
    cpl_ring[3].wait_recv()

    take_coupling(down)
    take_coupling(up)
    cpl_ring[4].wait_recv()
    cpl_ring[5].wait_recv()
    take_coupling(across)
    for copy in inv_ring + cpl_ring:
        copy.wait_send()

    def rows_of(step, index):
        return pl.ds(pl.multiple_of(index * step, step), step)

    def chunk(ref, rows):
        return ref[rows, :width], ref[rows, width:]

    def put(ref, rows, value):
        ref[rows, :width] = value[0]
        ref[rows, width:] = value[1]

    def plus(value, other):
        return value[0] + other[0], value[1] + other[1]

    next_odd = at(z, x_next, 1)

    def map_copy(index):
        rows = rows_of(map_step, index)
        return remote(
            map_out.at[rows], map_in.at[rows], map_send.at[index], map_recv.at[index], next_odd
        )

    def off_copy(index):
        rows = rows_of(off_step, index)
        return remote(
            off_out.at[rows], off_in.at[rows], off_send.at[index], off_recv.at[index], next_odd
        )

    maps = map_recv.shape[0]

    def whole_copy(kind, index):
        rows = rows_of(map_step, index)
        send, recv = whole_send.at[kind, index], whole_recv.at[kind, index]
        if kind < 2:
            return remote(map_out.at[rows], whole.at[col, rows], send, recv, (upward, downward)[kind])
        if index < maps // 2:
            return remote(whole.at[down, rows], whole.at[down, rows], send, recv, upward)
        return remote(whole.at[up, rows], whole.at[up, rows], send, recv, downward)

    def forward(index):
        whole_copy(0 if index < maps // 2 else 1, index).wait_recv()
        whole_copy(2, index).start()

    ends = off_recv.shape[0]
    early = ends // 2

    def first_copy(index):
        rows = rows_of(off_step, index)
        return remote(
            off_out.at[rows], z_in.at[rows], out_send.at[index], z_recv.at[index], at(1, 3, 1)
        )

    def offsets(index, count):
        rows = pl.ds(pl.multiple_of(index * off_step, off_step), count * off_step)
        for extra in range(count):
            off_copy(index + extra).wait_recv()
        value = product(*chunk(off_in, rows), pair_high, pair_low)
        put(off_out, rows, plus(value, chunk(offset, rows)))
        for extra in range(count):

            @pl.when(x < 3)
            def _():
                off_copy(index + extra).start()

            @pl.when((x == 3) & (z == 0))
            def _():
                first_copy(index + extra).start()

    hand_map = remote(map_in, map_in, core_send.at[ROWS + 1], core_recv.at[ROWS + 1], partner)
    hand_off = remote(off_in, off_in, core_send.at[ROWS + 2], core_recv.at[ROWS + 2], partner)

    @pl.when(core == 1)
    def _():
        def compose(which):
            rows = pl.ds(pl.multiple_of(which * block, block), block)
            even_map_copy(which).wait_recv()
            value = product(even_in[which, :, :width], even_in[which, :, width:], own_high, own_low)
            for part in range(2):
                high, low = split(value[part])
                pair_high[rows, part * width : (part + 1) * width] = high
                pair_low[rows, part * width : (part + 1) * width] = low
            return value

        first = compose(col)

        @pl.when(x == 0)
        def _():
            put(map_out, slice(None), first)
            for index in range(map_recv.shape[0]):
                map_copy(index).start()

        even_offset_copy.wait_recv()

        def compose_offset(index, carry):
            rows = rows_of(block, index)
            value = product(*chunk(even_offset, rows), own_high, own_low)
            put(offset, rows, plus(value, chunk(offset, rows)))
            return carry

        lax.fori_loop(0, columns // block, compose_offset, 0)

        @pl.when(x == 0)
        def _():
            off_out[...] = offset[...]
            for index in range(off_recv.shape[0]):
                off_copy(index).start()

        for which in (down, up, across):
            compose(which)

        @pl.when(x == 0)
        def _():
            for index in range(maps):
                whole_copy(0, index).start()
                whole_copy(1, index).start()
            for index in range(maps):
                forward(index)

        @pl.when(x > 0)
        def _():
            def map_sweep(index, carry):
                rows = rows_of(map_step, index)
                map_copy(index).wait_recv()
                put(map_out, rows, product(*chunk(map_in, rows), pair_high, pair_low))

                @pl.when(x < 3)
                def _():
                    map_copy(index).start()

                whole_copy(0, index).start()
                whole_copy(1, index).start()

                return carry

            lax.fori_loop(0, map_recv.shape[0], map_sweep, 0)

            def off_sweep(index, carry):
                offsets(index, 1)
                return carry

            done = 0
            for index in range(maps):
                until = max(0, index - maps // 2)
                if until > done:
                    lax.fori_loop(done, until, off_sweep, 0)
                    done = until
                forward(index)

            lax.fori_loop(done, early, off_sweep, 0)

            @pl.when((x < 3) | (z != 1))
            def _():
                lax.fori_loop(early, ends, off_sweep, 0)
                hand_map.start()
                hand_off.start()

        @pl.when(x < 3)
        def _():
            for index in range(map_recv.shape[0]):
                map_copy(index).wait_send()
            for index in range(off_recv.shape[0]):
                off_copy(index).wait_send()

    @pl.when(core == 0)
    def _():
        @pl.when(x == 0)
        def _():
            map_out[...] = even_map[col]
            off_out[...] = offset[...]

        @pl.when(x > 0)
        def _():
            hand_map.wait_recv()
            put(map_out, slice(None), product(*chunk(map_in, slice(None)), own_high, own_low))

        for index in range(maps):
            whole_copy(0, index).start()
            whole_copy(1, index).start()

        @pl.when(x > 0)
        def _():
            hand_off.wait_recv()

            def even_offsets(index, carry):
                rows = rows_of(block, index)
                value = product(*chunk(off_in, rows), own_high, own_low)
                put(off_out, rows, plus(value, chunk(offset, rows)))
                return carry

            lax.fori_loop(0, columns // block, even_offsets, 0)

        for index in range(maps):
            forward(index)

    def take_whole(which):
        rows = pl.ds(pl.multiple_of(which * block, block), block)
        high, low = split(whole[which])
        whole_high[rows] = high
        whole_low[rows] = low

    whole[col] = map_out[...]
    take_whole(col)
    for index in range(maps // 2, maps):
        whole_copy(0, index).wait_recv()
    take_whole(down)
    for index in range(maps // 2):
        whole_copy(1, index).wait_recv()
    take_whole(up)
    for index in range(maps):
        whole_copy(2, index).wait_recv()
    take_whole(across)
    for kind in range(3):
        for index in range(maps):
            whole_copy(kind, index).wait_send()

    def z_copy(index):
        rows = rows_of(end_step, index)
        return remote(
            state.at[rows], z_in.at[rows], out_send.at[index], z_recv.at[index], at((z + 1) % planes, 3, 1)
        )

    def enter_copy(index):
        rows = rows_of(end_step, index)
        return remote(
            z_in.at[rows], x_in.at[rows], pass_send.at[index], x_recv.at[index], at(z, 0, 1)
        )

    def enter_back_copy(index):
        rows = rows_of(end_step, index)
        return remote(
            z_in.at[rows], x_in.at[rows], back_send.at[index], x_recv.at[index], at(z, 2, 1)
        )

    def back_copy(index):
        rows = rows_of(end_step, index)
        return remote(
            x_in.at[rows], x_in.at[rows], back_send.at[index], x_recv.at[index], at(z, x_before, 1)
        )

    def pass_copy(index):
        rows = rows_of(end_step, index)
        return remote(
            x_in.at[rows], x_in.at[rows], pass_send.at[index], x_recv.at[index], partner
        )

    def enter_core_copy(index):
        rows = rows_of(end_step, index)
        return remote(
            z_in.at[rows], x_in.at[rows], core_pass.at[index], x_recv.at[index], partner
        )

    @pl.when((core == 1) & (x == 3))
    def _():
        @pl.when(z == 0)
        def _():
            z_in[...] = jnp.zeros_like(z_in)
            state[...] = off_out[...]
            for index in range(ends):
                enter_copy(index).start()
                enter_back_copy(index).start()
                enter_core_copy(index).start()

        @pl.when(z > 0)
        def _():
            def z_sweep(index, carry):
                rows = rows_of(end_step, index)
                z_copy(index).wait_recv()
                enter_copy(index).start()
                enter_back_copy(index).start()
                enter_core_copy(index).start()
                value = product(*chunk(z_in, rows), whole_high, whole_low)
                put(state, rows, plus(value, chunk(off_out, rows)))

                @pl.when(z < planes - 1)
                def _():
                    z_copy(index).start()

                return carry

            def both_sweep(index, carry):
                @pl.when(z == 1)
                def _():
                    offsets(early + 2 * index, 2)

                z_sweep(2 * index, carry)
                return z_sweep(2 * index + 1, carry)

            lax.fori_loop(0, (ends - early) // 2, both_sweep, 0)

            @pl.when(z == 1)
            def _():
                hand_map.start()
                hand_off.start()

            lax.fori_loop(ends - early, ends, z_sweep, 0)

        @pl.when(z < planes - 1)
        def _():
            for index in range(ends):
                z_copy(index).wait_send()

        for index in range(ends):
            enter_copy(index).wait_send()
            enter_back_copy(index).wait_send()
            enter_core_copy(index).wait_send()

    @pl.when((core == 0) | (x < 3))
    def _():
        def x_sweep(index, carry):
            pass_copy(index).wait_recv()

            @pl.when(odd & (x == 2))
            def _():
                back_copy(index).start()

            @pl.when(odd)
            def _():
                pass_copy(index).start()

            rows = rows_of(end_step, index)
            value = product(*chunk(x_in, rows), whole_high, whole_low)
            put(state, rows, plus(value, chunk(off_out, rows)))
            return carry

        lax.fori_loop(0, ends, x_sweep, 0)

        @pl.when(odd & (x == 2))
        def _():
            for index in range(ends):
                back_copy(index).wait_send()

        @pl.when(odd)
        def _():
            for index in range(ends):
                pass_copy(index).wait_send()

    @pl.when(odd & (x > 0))
    def _():
        hand_map.wait_send()
        hand_off.wait_send()

    @pl.when(core == 0)
    def _():
        for which in range(ROWS):
            even_map_copy(which).wait_send()
        even_offset_copy.wait_send()

    for start in range(0, columns, block):
        for part in range(2):
            out_ref[0, part, :, start : start + block] = state[
                start : start + block, part * width : (part + 1) * width
            ].T


def local(planes, inverses, couplings, sources, counts):
    width, block = inverses.shape[2], inverses.shape[3]
    columns = sources.shape[3]
    map_chunks, end_chunks = 8, 16
    single, half = jnp.float32, jnp.bfloat16
    vmem, dma = pltpu.VMEM, pltpu.SemaphoreType.DMA
    held_map = vmem((width, 2 * width), half)
    rows_buffer = vmem((columns, 2 * width), single)
    map_buffer = vmem((block, 2 * width), single)
    in_hbm = pl.BlockSpec(memory_space=pltpu.HBM)
    in_vmem = pl.BlockSpec(memory_space=pltpu.VMEM)
    return pl.pallas_call(
        functools.partial(kernel, planes),
        out_shape=jax.ShapeDtypeStruct(sources.shape, single),
        in_specs=[in_hbm, in_hbm, in_hbm, pl.BlockSpec(memory_space=pltpu.SMEM)],
        out_specs=in_vmem,
        scratch_shapes=[
            vmem((ROWS, 2, width, block), single),
            vmem((ROWS, 2, width, block), single),
            vmem((2, width, columns), single),
            held_map,
            held_map,
            held_map,
            held_map,
            held_map,
            held_map,
            vmem((ROWS, block, 2 * width), single),
            vmem((ROWS, block, 2 * width), single),
            rows_buffer,
            rows_buffer,
            map_buffer,
            map_buffer,
            rows_buffer,
            rows_buffer,
            vmem((ROWS, block, 2 * width), single),
            held_map,
            held_map,
            rows_buffer,
            rows_buffer,
            rows_buffer,
            dma((3,)),
            dma((2, 6)),
            dma((2, 6)),
            dma((ROWS + 3,)),
            dma((ROWS + 3,)),
            dma((map_chunks,)),
            dma((map_chunks,)),
            dma((end_chunks,)),
            dma((end_chunks,)),
            dma((end_chunks,)),
            dma((end_chunks,)),
            dma((end_chunks,)),
            dma((end_chunks,)),
            dma((end_chunks,)),
            dma((3, map_chunks)),
            dma((3, map_chunks)),
            dma((end_chunks,)),
            pltpu.SemaphoreType.REGULAR,
        ],
        compiler_params=pltpu.CompilerParams(
            collective_id=0, has_side_effects=True, vmem_limit_bytes=40 * 2**20
        ),
    )(*(pltpu.with_memory_space_constraint(v, pltpu.HBM) for v in (inverses, couplings, sources)), counts)


def solution(mesh):
    placed = (
        P("chain", None, None, "col"),
        P("chain", None, None, "col"),
        P("chain", None, None, "col"),
        P("chain"),
    )
    return jax.shard_map(
        functools.partial(local, mesh.shape["chain"] // PLANE),
        mesh=mesh,
        in_specs=placed,
        out_specs=P("chain", None, None, "col"),
        check_vma=False,
    )
```

```python
import functools

import jax
import jax.numpy as jnp
from jax import lax
from jax.experimental import pallas as pl
from jax.experimental.pallas import tpu as pltpu
from jax.sharding import PartitionSpec as P

MESH = pl.DeviceIdType.MESH
PLANE = 8
ROWS = 4


def split(value):
    high = value.astype(jnp.bfloat16)
    return high, (value - high.astype(jnp.float32)).astype(jnp.bfloat16)


def product(real, imag, high_ref, low_ref):
    count, width = real.shape
    tile = min(256, width)
    real_high, real_low = split(real)
    imag_high, imag_low = split(imag)
    high = jnp.concatenate([real_high, imag_high], axis=0)
    both = jnp.concatenate([real_high, imag_high, real_low, imag_low], axis=0)

    def against(columns):
        wide = jnp.dot(both, high_ref[:, columns], preferred_element_type=jnp.float32)
        narrow = jnp.dot(high, low_ref[:, columns], preferred_element_type=jnp.float32)
        return wide[: 2 * count] + (wide[2 * count :] + narrow)

    reals, imags = [], []
    for start in range(0, width, tile):
        by_real = against(slice(start, start + tile))
        by_imag = against(slice(width + start, width + start + tile))
        reals.append(by_real[:count] - by_imag[count:])
        imags.append(by_imag[:count] + by_real[count:])
    return jnp.concatenate(reals, axis=1), jnp.concatenate(imags, axis=1)


def kernel(
    planes,
    inverse_ref,
    coupling_ref,
    source_ref,
    count_ref,
    out_ref,
    inv,
    cpl,
    src,
    inv_high,
    inv_low,
    own_high,
    own_low,
    pair_high,
    pair_low,
    even_map,
    even_in,
    even_offset,
    offset,
    map_in,
    map_out,
    off_in,
    off_out,
    whole,
    whole_high,
    whole_low,
    z_in,
    x_in,
    state,
    local_sem,
    gather_send,
    gather_recv,
    core_send,
    core_recv,
    map_send,
    map_recv,
    off_send,
    off_recv,
    z_recv,
    x_recv,
    out_send,
    pass_send,
    back_send,
    whole_send,
    whole_recv,
    core_pass,
    turn_sem,
):
    width = inv_high.shape[0]
    block = width // ROWS
    columns = offset.shape[0]
    map_step = block // map_recv.shape[0]
    off_step = columns // off_recv.shape[0]
    end_step = columns // z_recv.shape[0]

    place = lax.axis_index("chain")
    col = lax.axis_index("col")
    z = place // PLANE
    x = (place % PLANE) // 2
    core = place % 2
    up, down, across = (col + 1) % ROWS, (col + 3) % ROWS, (col + 2) % ROWS

    def at(z_to, x_to, core_to):
        return {"chain": z_to * PLANE + x_to * 2 + core_to, "col": col}

    partner = at(z, x, 1 - core)
    upward = {"chain": place, "col": up}
    downward = {"chain": place, "col": down}
    x_next, x_before = (x + 1) % 4, (x + 3) % 4
    odd, last = core == 1, (core == 1) & (x == 3)

    own_inv = pltpu.make_async_copy(inverse_ref.at[0], inv.at[col], local_sem.at[0])
    own_cpl = pltpu.make_async_copy(coupling_ref.at[0], cpl.at[col], local_sem.at[1])
    own_src = pltpu.make_async_copy(source_ref.at[0], src, local_sem.at[2])
    own_inv.start()
    own_cpl.start()
    own_src.start()

    barrier = pltpu.get_barrier_semaphore()

    def greet(when, device):
        @pl.when(when)
        def _():
            pl.semaphore_signal(barrier, inc=1, device_id=device, device_id_type=MESH)

        return jnp.where(when, 1, 0)

    for device in (upward, downward, partner):
        pl.semaphore_signal(barrier, inc=1, device_id=device, device_id_type=MESH)
    greeted = 3
    greeted += greet(odd, at(z, x_next, 1))
    greeted += greet(odd, at(z, x_before, 1))
    greeted += greet(last & (z < planes - 1), at(z + 1, 3, 1))
    greeted += greet(last & (z > 0), at(z - 1, 3, 1))
    pl.semaphore_wait(barrier, greeted)

    def remote(source, target, send, recv, device):
        return pltpu.make_async_remote_copy(
            src_ref=source,
            dst_ref=target,
            send_sem=send,
            recv_sem=recv,
            device_id=device,
            device_id_type=MESH,
        )

    def ring(held, which):
        send, recv = gather_send.at[which], gather_recv.at[which]
        first, second = held.at[:, 0], held.at[:, 1]
        own_first, own_second = first.at[col], second.at[col]
        return [
            remote(own_first, first.at[col], send.at[0], recv.at[0], upward),
            remote(own_second, second.at[col], send.at[1], recv.at[1], downward),
            remote(own_second, second.at[col], send.at[2], recv.at[2], upward),
            remote(own_first, first.at[col], send.at[3], recv.at[3], downward),
            remote(first.at[down], first.at[down], send.at[4], recv.at[4], upward),
            remote(second.at[up], second.at[up], send.at[5], recv.at[5], downward),
        ]

    inv_ring = ring(inv, 0)
    cpl_ring = ring(cpl, 1)
    @pl.when(core == 0)
    def _():
        pl.semaphore_wait(turn_sem, 1)

    own_inv.wait()
    for copy in inv_ring[:4]:
        copy.start()

    active = (lax.broadcasted_iota(jnp.int32, (1, width), 1) < count_ref[0]).astype(jnp.float32)

    def take_inverse(which):
        rows = pl.ds(pl.multiple_of(which * block, block), block)
        for part in range(2):
            high, low = split(inv[which, part].T * active)
            inv_high[rows, part * width : (part + 1) * width] = high
            inv_low[rows, part * width : (part + 1) * width] = low

    take_inverse(col)
    inv_ring[0].wait_recv()
    inv_ring[4].start()
    inv_ring[1].wait_recv()
    inv_ring[5].start()
    own_cpl.wait()
    for copy in cpl_ring[:4]:
        copy.start()

    @pl.when(core == 1)
    def _():
        pl.semaphore_signal(turn_sem, inc=1, device_id=partner, device_id_type=MESH)

    inv_ring[2].wait_recv()
    take_inverse(down)
    inv_ring[3].wait_recv()
    take_inverse(up)
    inv_ring[4].wait_recv()
    inv_ring[5].wait_recv()
    take_inverse(across)

    def even_map_copy(which, half):
        rows = slice(half * block // 2, (half + 1) * block // 2)
        return remote(
            even_map.at[which, rows],
            even_in.at[which, rows],
            core_send.at[which, half],
            core_recv.at[which, half],
            partner,
        )

    def take_coupling(which, start=0, size=block):
        rows = pl.ds(pl.multiple_of(which * block + start, size), size)
        part_rows = slice(start, start + size)
        real, imag = product(
            cpl[which, 0].T[part_rows], cpl[which, 1].T[part_rows], inv_high, inv_low
        )
        for part, value in enumerate((real, imag)):
            high, low = split(value)
            own_high[rows, part * width : (part + 1) * width] = high
            own_low[rows, part * width : (part + 1) * width] = low

        @pl.when(core == 0)
        def _():
            even_map[which, part_rows, :width] = real
            even_map[which, part_rows, width:] = imag
            for half in range(2 * start // block, 2 * (start + size) // block):
                even_map_copy(which, half).start()

    take_coupling(col)
    own_src.wait()
    for start in range(0, columns, block):
        real, imag = product(
            src[0, :, start : start + block].T, src[1, :, start : start + block].T, inv_high, inv_low
        )
        offset[start : start + block, :width] = real
        offset[start : start + block, width:] = imag

    even_offset_copy = remote(offset, even_offset, core_send.at[ROWS, 0], core_recv.at[ROWS, 0], partner)

    @pl.when(core == 0)
    def _():
        even_offset_copy.start()

    cpl_ring[0].wait_recv()
    cpl_ring[4].start()
    cpl_ring[1].wait_recv()
    cpl_ring[5].start()
    cpl_ring[2].wait_recv()
    cpl_ring[3].wait_recv()

    take_coupling(down)
    take_coupling(up)
    cpl_ring[4].wait_recv()
    cpl_ring[5].wait_recv()
    take_coupling(across, 0, block // 2)
    take_coupling(across, block // 2, block // 2)
    for copy in inv_ring + cpl_ring:
        copy.wait_send()

    def rows_of(step, index):
        return pl.ds(pl.multiple_of(index * step, step), step)

    def chunk(ref, rows):
        return ref[rows, :width], ref[rows, width:]

    def put(ref, rows, value):
        ref[rows, :width] = value[0]
        ref[rows, width:] = value[1]

    def plus(value, other):
        return value[0] + other[0], value[1] + other[1]

    next_odd = at(z, x_next, 1)

    def map_copy(index):
        rows = rows_of(map_step, index)
        return remote(
            map_out.at[rows], map_in.at[rows], map_send.at[index], map_recv.at[index], next_odd
        )

    def off_copy(index):
        rows = rows_of(off_step, index)
        return remote(
            off_out.at[rows], off_in.at[rows], off_send.at[index], off_recv.at[index], next_odd
        )

    maps = map_recv.shape[0]

    def whole_copy(kind, index):
        rows = rows_of(map_step, index)
        send, recv = whole_send.at[kind, index], whole_recv.at[kind, index]
        if kind < 2:
            return remote(map_out.at[rows], whole.at[col, rows], send, recv, (upward, downward)[kind])
        if index < maps // 2:
            return remote(whole.at[down, rows], whole.at[down, rows], send, recv, upward)
        return remote(whole.at[up, rows], whole.at[up, rows], send, recv, downward)

    def forward(index):
        whole_copy(0 if index < maps // 2 else 1, index).wait_recv()
        whole_copy(2, index).start()

    ends = off_recv.shape[0]
    early = ends // 2

    def first_copy(index):
        rows = rows_of(off_step, index)
        return remote(
            off_out.at[rows], z_in.at[rows], out_send.at[index], z_recv.at[index], at(1, 3, 1)
        )

    def offsets(index, count):
        rows = pl.ds(pl.multiple_of(index * off_step, off_step), count * off_step)
        for extra in range(count):
            off_copy(index + extra).wait_recv()
        value = product(*chunk(off_in, rows), pair_high, pair_low)
        put(off_out, rows, plus(value, chunk(offset, rows)))
        for extra in range(count):

            @pl.when(x < 3)
            def _():
                off_copy(index + extra).start()

            @pl.when((x == 3) & (z == 0))
            def _():
                first_copy(index + extra).start()

    hand_map = remote(map_in, map_in, core_send.at[ROWS + 1, 0], core_recv.at[ROWS + 1, 0], partner)
    hand_off = remote(off_in, off_in, core_send.at[ROWS + 2, 0], core_recv.at[ROWS + 2, 0], partner)

    @pl.when(core == 1)
    def _():
        def compose(which, start=0, size=block):
            rows = pl.ds(pl.multiple_of(which * block + start, size), size)
            part_rows = slice(start, start + size)
            for half in range(2 * start // block, 2 * (start + size) // block):
                even_map_copy(which, half).wait_recv()
            value = product(
                even_in[which, part_rows, :width], even_in[which, part_rows, width:], own_high, own_low
            )
            for part in range(2):
                high, low = split(value[part])
                pair_high[rows, part * width : (part + 1) * width] = high
                pair_low[rows, part * width : (part + 1) * width] = low
            return value

        first = compose(col)

        @pl.when(x == 0)
        def _():
            put(map_out, slice(None), first)
            for index in range(map_recv.shape[0]):
                map_copy(index).start()

        even_offset_copy.wait_recv()

        def compose_offset(index, carry):
            rows = rows_of(block, index)
            value = product(*chunk(even_offset, rows), own_high, own_low)
            put(offset, rows, plus(value, chunk(offset, rows)))
            return carry

        lax.fori_loop(0, columns // block, compose_offset, 0)

        @pl.when(x == 0)
        def _():
            off_out[...] = offset[...]
            for index in range(off_recv.shape[0]):
                off_copy(index).start()

        for which in (down, up):
            compose(which)
        compose(across, 0, block // 2)
        compose(across, block // 2, block // 2)

        @pl.when(x == 0)
        def _():
            for index in range(maps):
                whole_copy(0, index).start()
                whole_copy(1, index).start()
            for index in range(maps):
                forward(index)

        @pl.when(x > 0)
        def _():
            def map_sweep(index, carry):
                rows = rows_of(map_step, index)
                map_copy(index).wait_recv()
                put(map_out, rows, product(*chunk(map_in, rows), pair_high, pair_low))

                @pl.when(x < 3)
                def _():
                    map_copy(index).start()

                whole_copy(0, index).start()
                whole_copy(1, index).start()

                return carry

            lax.fori_loop(0, map_recv.shape[0], map_sweep, 0)

            def off_sweep(index, carry):
                offsets(index, 1)
                return carry

            done = 0
            for index in range(maps):
                until = max(0, index - maps // 2)
                if until > done:
                    lax.fori_loop(done, until, off_sweep, 0)
                    done = until
                forward(index)

            lax.fori_loop(done, early, off_sweep, 0)

            @pl.when((x < 3) | (z != 1))
            def _():
                lax.fori_loop(early, ends, off_sweep, 0)
                hand_map.start()
                hand_off.start()

        @pl.when(x < 3)
        def _():
            for index in range(map_recv.shape[0]):
                map_copy(index).wait_send()
            for index in range(off_recv.shape[0]):
                off_copy(index).wait_send()

    @pl.when(core == 0)
    def _():
        @pl.when(x == 0)
        def _():
            map_out[...] = even_map[col]
            off_out[...] = offset[...]

        @pl.when(x > 0)
        def _():
            hand_map.wait_recv()
            put(map_out, slice(None), product(*chunk(map_in, slice(None)), own_high, own_low))

        for index in range(maps):
            whole_copy(0, index).start()
            whole_copy(1, index).start()

        @pl.when(x > 0)
        def _():
            hand_off.wait_recv()

            def even_offsets(index, carry):
                rows = rows_of(block, index)
                value = product(*chunk(off_in, rows), own_high, own_low)
                put(off_out, rows, plus(value, chunk(offset, rows)))
                return carry

            lax.fori_loop(0, columns // block, even_offsets, 0)

        for index in range(maps):
            forward(index)

    def take_whole(which):
        rows = pl.ds(pl.multiple_of(which * block, block), block)
        high, low = split(whole[which])
        whole_high[rows] = high
        whole_low[rows] = low

    whole[col] = map_out[...]
    take_whole(col)
    for index in range(maps // 2, maps):
        whole_copy(0, index).wait_recv()
    take_whole(down)
    for index in range(maps // 2):
        whole_copy(1, index).wait_recv()
    take_whole(up)
    for index in range(maps):
        whole_copy(2, index).wait_recv()
    take_whole(across)
    for kind in range(3):
        for index in range(maps):
            whole_copy(kind, index).wait_send()

    def z_copy(index):
        rows = rows_of(end_step, index)
        return remote(
            state.at[rows], z_in.at[rows], out_send.at[index], z_recv.at[index], at((z + 1) % planes, 3, 1)
        )

    def enter_copy(index):
        rows = rows_of(end_step, index)
        return remote(
            z_in.at[rows], x_in.at[rows], pass_send.at[index], x_recv.at[index], at(z, 0, 1)
        )

    def enter_back_copy(index):
        rows = rows_of(end_step, index)
        return remote(
            z_in.at[rows], x_in.at[rows], back_send.at[index], x_recv.at[index], at(z, 2, 1)
        )

    def back_copy(index):
        rows = rows_of(end_step, index)
        return remote(
            x_in.at[rows], x_in.at[rows], back_send.at[index], x_recv.at[index], at(z, x_before, 1)
        )

    def pass_copy(index):
        rows = rows_of(end_step, index)
        return remote(
            x_in.at[rows], x_in.at[rows], pass_send.at[index], x_recv.at[index], partner
        )

    def enter_core_copy(index):
        rows = rows_of(end_step, index)
        return remote(
            z_in.at[rows], x_in.at[rows], core_pass.at[index], x_recv.at[index], partner
        )

    @pl.when((core == 1) & (x == 3))
    def _():
        @pl.when(z == 0)
        def _():
            z_in[...] = jnp.zeros_like(z_in)
            state[...] = off_out[...]
            for index in range(ends):
                enter_copy(index).start()
                enter_back_copy(index).start()
                enter_core_copy(index).start()

        @pl.when(z > 0)
        def _():
            def z_sweep(index, carry):
                rows = rows_of(end_step, index)
                z_copy(index).wait_recv()
                enter_copy(index).start()
                enter_back_copy(index).start()
                enter_core_copy(index).start()
                value = product(*chunk(z_in, rows), whole_high, whole_low)
                put(state, rows, plus(value, chunk(off_out, rows)))

                @pl.when(z < planes - 1)
                def _():
                    z_copy(index).start()

                return carry

            def both_sweep(index, carry):
                @pl.when(z == 1)
                def _():
                    offsets(early + 2 * index, 2)

                z_sweep(2 * index, carry)
                return z_sweep(2 * index + 1, carry)

            lax.fori_loop(0, (ends - early) // 2, both_sweep, 0)

            @pl.when(z == 1)
            def _():
                hand_map.start()
                hand_off.start()

            lax.fori_loop(ends - early, ends, z_sweep, 0)

        @pl.when(z < planes - 1)
        def _():
            for index in range(ends):
                z_copy(index).wait_send()

        for index in range(ends):
            enter_copy(index).wait_send()
            enter_back_copy(index).wait_send()
            enter_core_copy(index).wait_send()

    def give(piece):
        rows = slice(piece * block, (piece + 1) * block)
        for part in range(2):
            out_ref[0, part, :, rows] = state[rows, part * width : (part + 1) * width].T

    @pl.when((core == 0) | (x < 3))
    def _():
        def x_sweep(index, carry):
            pass_copy(index).wait_recv()

            @pl.when(odd & (x == 2))
            def _():
                back_copy(index).start()

            @pl.when(odd)
            def _():
                pass_copy(index).start()

            rows = rows_of(end_step, index)
            value = product(*chunk(x_in, rows), whole_high, whole_low)
            put(state, rows, plus(value, chunk(off_out, rows)))
            return carry

        pieces = columns // block
        for piece in range(pieces):
            lax.fori_loop(piece * ends // pieces, (piece + 1) * ends // pieces, x_sweep, 0)
            give(piece)

        @pl.when(odd & (x == 2))
        def _():
            for index in range(ends):
                back_copy(index).wait_send()

        @pl.when(odd)
        def _():
            for index in range(ends):
                pass_copy(index).wait_send()

    @pl.when(odd & (x > 0))
    def _():
        hand_map.wait_send()
        hand_off.wait_send()

    @pl.when(core == 0)
    def _():
        for which in range(ROWS):
            even_map_copy(which, 0).wait_send()
            even_map_copy(which, 1).wait_send()
        even_offset_copy.wait_send()

    @pl.when(last)
    def _():
        for piece in range(columns // block):
            give(piece)


def local(planes, inverses, couplings, sources, counts):
    width, block = inverses.shape[2], inverses.shape[3]
    columns = sources.shape[3]
    map_chunks, end_chunks = 8, 16
    single, half = jnp.float32, jnp.bfloat16
    vmem, dma = pltpu.VMEM, pltpu.SemaphoreType.DMA
    held_map = vmem((width, 2 * width), half)
    rows_buffer = vmem((columns, 2 * width), single)
    map_buffer = vmem((block, 2 * width), single)
    in_hbm = pl.BlockSpec(memory_space=pltpu.HBM)
    in_vmem = pl.BlockSpec(memory_space=pltpu.VMEM)
    return pl.pallas_call(
        functools.partial(kernel, planes),
        out_shape=jax.ShapeDtypeStruct(sources.shape, single),
        in_specs=[in_hbm, in_hbm, in_hbm, pl.BlockSpec(memory_space=pltpu.SMEM)],
        out_specs=in_vmem,
        scratch_shapes=[
            vmem((ROWS, 2, width, block), single),
            vmem((ROWS, 2, width, block), single),
            vmem((2, width, columns), single),
            held_map,
            held_map,
            held_map,
            held_map,
            held_map,
            held_map,
            vmem((ROWS, block, 2 * width), single),
            vmem((ROWS, block, 2 * width), single),
            rows_buffer,
            rows_buffer,
            map_buffer,
            map_buffer,
            rows_buffer,
            rows_buffer,
            vmem((ROWS, block, 2 * width), single),
            held_map,
            held_map,
            rows_buffer,
            rows_buffer,
            rows_buffer,
            dma((3,)),
            dma((2, 6)),
            dma((2, 6)),
            dma((ROWS + 3, 2)),
            dma((ROWS + 3, 2)),
            dma((map_chunks,)),
            dma((map_chunks,)),
            dma((end_chunks,)),
            dma((end_chunks,)),
            dma((end_chunks,)),
            dma((end_chunks,)),
            dma((end_chunks,)),
            dma((end_chunks,)),
            dma((end_chunks,)),
            dma((3, map_chunks)),
            dma((3, map_chunks)),
            dma((end_chunks,)),
            pltpu.SemaphoreType.REGULAR,
        ],
        compiler_params=pltpu.CompilerParams(
            collective_id=0, has_side_effects=True, vmem_limit_bytes=40 * 2**20
        ),
    )(*(pltpu.with_memory_space_constraint(v, pltpu.HBM) for v in (inverses, couplings, sources)), counts)


def solution(mesh):
    placed = (
        P("chain", None, None, "col"),
        P("chain", None, None, "col"),
        P("chain", None, None, "col"),
        P("chain"),
    )
    return jax.shard_map(
        functools.partial(local, mesh.shape["chain"] // PLANE),
        mesh=mesh,
        in_specs=placed,
        out_specs=P("chain", None, None, "col"),
        check_vma=False,
    )
```

```python
import functools

import jax
import jax.numpy as jnp
from jax import lax
from jax.experimental import pallas as pl
from jax.experimental.pallas import tpu as pltpu
from jax.sharding import PartitionSpec as P

MESH = pl.DeviceIdType.MESH
PLANE = 8
ROWS = 4


def split(value):
    high = value.astype(jnp.bfloat16)
    return high, (value - high.astype(jnp.float32)).astype(jnp.bfloat16)


def product(real, imag, high_ref, low_ref):
    count, width = real.shape
    tile = min(256, width)
    real_high, real_low = split(real)
    imag_high, imag_low = split(imag)
    high = jnp.concatenate([real_high, imag_high], axis=0)
    both = jnp.concatenate([real_high, imag_high, real_low, imag_low], axis=0)

    def against(columns):
        wide = jnp.dot(both, high_ref[:, columns], preferred_element_type=jnp.float32)
        narrow = jnp.dot(high, low_ref[:, columns], preferred_element_type=jnp.float32)
        return wide[: 2 * count] + (wide[2 * count :] + narrow)

    reals, imags = [], []
    for start in range(0, width, tile):
        by_real = against(slice(start, start + tile))
        by_imag = against(slice(width + start, width + start + tile))
        reals.append(by_real[:count] - by_imag[count:])
        imags.append(by_imag[:count] + by_real[count:])
    return jnp.concatenate(reals, axis=1), jnp.concatenate(imags, axis=1)


def kernel(
    planes,
    inverse_ref,
    coupling_ref,
    source_ref,
    count_ref,
    out_ref,
    inv,
    cpl,
    src,
    inv_high,
    inv_low,
    own_high,
    own_low,
    pair_high,
    pair_low,
    even_map,
    even_in,
    even_offset,
    offset,
    map_in,
    map_out,
    off_in,
    off_out,
    whole,
    whole_high,
    whole_low,
    z_in,
    x_in,
    state,
    local_sem,
    gather_send,
    gather_recv,
    core_send,
    core_recv,
    map_send,
    map_recv,
    off_send,
    off_recv,
    z_recv,
    x_recv,
    out_send,
    pass_send,
    back_send,
    whole_send,
    whole_recv,
    core_pass,
    turn_sem,
):
    width = inv_high.shape[0]
    block = width // ROWS
    columns = offset.shape[0]
    map_step = block // map_recv.shape[0]
    off_step = columns // off_recv.shape[0]
    end_step = columns // z_recv.shape[0]

    place = lax.axis_index("chain")
    col = lax.axis_index("col")
    z = place // PLANE
    x = (place % PLANE) // 2
    core = place % 2
    up, down, across = (col + 1) % ROWS, (col + 3) % ROWS, (col + 2) % ROWS

    def at(z_to, x_to, core_to):
        return {"chain": z_to * PLANE + x_to * 2 + core_to, "col": col}

    partner = at(z, x, 1 - core)
    upward = {"chain": place, "col": up}
    downward = {"chain": place, "col": down}
    x_next, x_before = (x + 1) % 4, (x + 3) % 4
    odd, last = core == 1, (core == 1) & (x == 3)

    own_inv = pltpu.make_async_copy(inverse_ref.at[0], inv.at[col], local_sem.at[0])
    own_cpl = pltpu.make_async_copy(coupling_ref.at[0], cpl.at[col], local_sem.at[1])
    own_src = pltpu.make_async_copy(source_ref.at[0], src, local_sem.at[2])
    own_inv.start()
    own_cpl.start()
    own_src.start()

    barrier = pltpu.get_barrier_semaphore()

    def greet(when, device):
        @pl.when(when)
        def _():
            pl.semaphore_signal(barrier, inc=1, device_id=device, device_id_type=MESH)

        return jnp.where(when, 1, 0)

    for device in (upward, downward, partner):
        pl.semaphore_signal(barrier, inc=1, device_id=device, device_id_type=MESH)
    greeted = 3
    greeted += greet(odd, at(z, x_next, 1))
    greeted += greet(odd, at(z, x_before, 1))
    greeted += greet(last & (z < planes - 1), at(z + 1, 3, 1))
    greeted += greet(last & (z > 0), at(z - 1, 3, 1))
    pl.semaphore_wait(barrier, greeted)

    def remote(source, target, send, recv, device):
        return pltpu.make_async_remote_copy(
            src_ref=source,
            dst_ref=target,
            send_sem=send,
            recv_sem=recv,
            device_id=device,
            device_id_type=MESH,
        )

    def ring(held, which):
        send, recv = gather_send.at[which], gather_recv.at[which]
        first, second = held.at[:, 0], held.at[:, 1]
        own_first, own_second = first.at[col], second.at[col]
        return [
            remote(own_first, first.at[col], send.at[0], recv.at[0], upward),
            remote(own_second, second.at[col], send.at[1], recv.at[1], downward),
            remote(own_second, second.at[col], send.at[2], recv.at[2], upward),
            remote(own_first, first.at[col], send.at[3], recv.at[3], downward),
            remote(first.at[down], first.at[down], send.at[4], recv.at[4], upward),
            remote(second.at[up], second.at[up], send.at[5], recv.at[5], downward),
        ]

    inv_ring = ring(inv, 0)
    cpl_ring = ring(cpl, 1)
    own_inv.wait()
    for copy in inv_ring[:4]:
        copy.start()

    active = (lax.broadcasted_iota(jnp.int32, (1, width), 1) < count_ref[0]).astype(jnp.float32)

    def take_inverse(which):
        rows = pl.ds(pl.multiple_of(which * block, block), block)
        for part in range(2):
            high, low = split(inv[which, part].T * active)
            inv_high[rows, part * width : (part + 1) * width] = high
            inv_low[rows, part * width : (part + 1) * width] = low

    take_inverse(col)
    inv_ring[0].wait_recv()
    inv_ring[4].start()
    inv_ring[1].wait_recv()
    inv_ring[5].start()
    own_cpl.wait()

    @pl.when(core == 0)
    def _():
        pl.semaphore_wait(turn_sem, 1)

    for copy in cpl_ring[:4]:
        copy.start()

    inv_ring[2].wait_recv()
    take_inverse(down)
    inv_ring[3].wait_recv()
    take_inverse(up)
    inv_ring[4].wait_recv()
    inv_ring[5].wait_recv()
    take_inverse(across)

    def even_map_copy(which, half):
        rows = slice(half * block // 2, (half + 1) * block // 2)
        return remote(
            even_map.at[which, rows],
            even_in.at[which, rows],
            core_send.at[which, half],
            core_recv.at[which, half],
            partner,
        )

    def take_coupling(which, start=0, size=block):
        rows = pl.ds(pl.multiple_of(which * block + start, size), size)
        part_rows = slice(start, start + size)
        real, imag = product(
            cpl[which, 0].T[part_rows], cpl[which, 1].T[part_rows], inv_high, inv_low
        )
        for part, value in enumerate((real, imag)):
            high, low = split(value)
            own_high[rows, part * width : (part + 1) * width] = high
            own_low[rows, part * width : (part + 1) * width] = low

        @pl.when(core == 0)
        def _():
            even_map[which, part_rows, :width] = real
            even_map[which, part_rows, width:] = imag
            for half in range(2 * start // block, 2 * (start + size) // block):
                even_map_copy(which, half).start()

    take_coupling(col)
    own_src.wait()
    for start in range(0, columns, block):
        real, imag = product(
            src[0, :, start : start + block].T, src[1, :, start : start + block].T, inv_high, inv_low
        )
        offset[start : start + block, :width] = real
        offset[start : start + block, width:] = imag

    even_offset_copy = remote(offset, even_offset, core_send.at[ROWS, 0], core_recv.at[ROWS, 0], partner)

    @pl.when(core == 0)
    def _():
        even_offset_copy.start()

    cpl_ring[0].wait_recv()
    cpl_ring[4].start()
    cpl_ring[1].wait_recv()
    cpl_ring[5].start()

    @pl.when(core == 1)
    def _():
        pl.semaphore_signal(turn_sem, inc=1, device_id=partner, device_id_type=MESH)

    cpl_ring[2].wait_recv()
    cpl_ring[3].wait_recv()

    take_coupling(down)
    take_coupling(up)
    cpl_ring[4].wait_recv()
    cpl_ring[5].wait_recv()
    take_coupling(across, 0, block // 2)
    take_coupling(across, block // 2, block // 2)
    for copy in inv_ring + cpl_ring:
        copy.wait_send()

    def rows_of(step, index):
        return pl.ds(pl.multiple_of(index * step, step), step)

    def chunk(ref, rows):
        return ref[rows, :width], ref[rows, width:]

    def put(ref, rows, value):
        ref[rows, :width] = value[0]
        ref[rows, width:] = value[1]

    def plus(value, other):
        return value[0] + other[0], value[1] + other[1]

    next_odd = at(z, x_next, 1)

    def map_copy(index):
        rows = rows_of(map_step, index)
        return remote(
            map_out.at[rows], map_in.at[rows], map_send.at[index], map_recv.at[index], next_odd
        )

    def off_copy(index):
        rows = rows_of(off_step, index)
        return remote(
            off_out.at[rows], off_in.at[rows], off_send.at[index], off_recv.at[index], next_odd
        )

    maps = map_recv.shape[0]

    def whole_copy(kind, index):
        rows = rows_of(map_step, index)
        send, recv = whole_send.at[kind, index], whole_recv.at[kind, index]
        if kind < 2:
            return remote(map_out.at[rows], whole.at[col, rows], send, recv, (upward, downward)[kind])
        if index < maps // 2:
            return remote(whole.at[down, rows], whole.at[down, rows], send, recv, upward)
        return remote(whole.at[up, rows], whole.at[up, rows], send, recv, downward)

    def forward(index):
        whole_copy(0 if index < maps // 2 else 1, index).wait_recv()
        whole_copy(2, index).start()

    ends = off_recv.shape[0]
    early = ends // 2

    def first_copy(index):
        rows = rows_of(off_step, index)
        return remote(
            off_out.at[rows], z_in.at[rows], out_send.at[index], z_recv.at[index], at(1, 3, 1)
        )

    def offsets(index, count):
        rows = pl.ds(pl.multiple_of(index * off_step, off_step), count * off_step)
        for extra in range(count):
            off_copy(index + extra).wait_recv()
        value = product(*chunk(off_in, rows), pair_high, pair_low)
        put(off_out, rows, plus(value, chunk(offset, rows)))
        for extra in range(count):

            @pl.when(x < 3)
            def _():
                off_copy(index + extra).start()

            @pl.when((x == 3) & (z == 0))
            def _():
                first_copy(index + extra).start()

    hand_map = remote(map_in, map_in, core_send.at[ROWS + 1, 0], core_recv.at[ROWS + 1, 0], partner)
    hand_off = remote(off_in, off_in, core_send.at[ROWS + 2, 0], core_recv.at[ROWS + 2, 0], partner)

    @pl.when(core == 1)
    def _():
        def compose(which, start=0, size=block):
            rows = pl.ds(pl.multiple_of(which * block + start, size), size)
            part_rows = slice(start, start + size)
            for half in range(2 * start // block, 2 * (start + size) // block):
                even_map_copy(which, half).wait_recv()
            value = product(
                even_in[which, part_rows, :width], even_in[which, part_rows, width:], own_high, own_low
            )
            for part in range(2):
                high, low = split(value[part])
                pair_high[rows, part * width : (part + 1) * width] = high
                pair_low[rows, part * width : (part + 1) * width] = low
            return value

        first = compose(col)

        @pl.when(x == 0)
        def _():
            put(map_out, slice(None), first)
            for index in range(map_recv.shape[0]):
                map_copy(index).start()

        even_offset_copy.wait_recv()

        def compose_offset(index, carry):
            rows = rows_of(block, index)
            value = product(*chunk(even_offset, rows), own_high, own_low)
            put(offset, rows, plus(value, chunk(offset, rows)))
            return carry

        lax.fori_loop(0, columns // block, compose_offset, 0)

        @pl.when(x == 0)
        def _():
            off_out[...] = offset[...]
            for index in range(off_recv.shape[0]):
                off_copy(index).start()

        for which in (down, up):
            compose(which)
        compose(across, 0, block // 2)
        compose(across, block // 2, block // 2)

        @pl.when(x == 0)
        def _():
            for index in range(maps):
                whole_copy(0, index).start()
                whole_copy(1, index).start()
            for index in range(maps):
                forward(index)

        @pl.when(x > 0)
        def _():
            def map_sweep(index, carry):
                rows = rows_of(map_step, index)
                map_copy(index).wait_recv()
                put(map_out, rows, product(*chunk(map_in, rows), pair_high, pair_low))

                @pl.when(x < 3)
                def _():
                    map_copy(index).start()

                whole_copy(0, index).start()
                whole_copy(1, index).start()

                return carry

            lax.fori_loop(0, map_recv.shape[0], map_sweep, 0)

            def off_sweep(index, carry):
                offsets(index, 1)
                return carry

            done = 0
            for index in range(maps):
                until = max(0, index - maps // 2)
                if until > done:
                    lax.fori_loop(done, until, off_sweep, 0)
                    done = until
                forward(index)

            lax.fori_loop(done, early, off_sweep, 0)

            @pl.when((x < 3) | (z != 1))
            def _():
                lax.fori_loop(early, ends, off_sweep, 0)
                hand_map.start()
                hand_off.start()

        @pl.when(x < 3)
        def _():
            for index in range(map_recv.shape[0]):
                map_copy(index).wait_send()
            for index in range(off_recv.shape[0]):
                off_copy(index).wait_send()

    @pl.when(core == 0)
    def _():
        @pl.when(x == 0)
        def _():
            map_out[...] = even_map[col]
            off_out[...] = offset[...]

        @pl.when(x > 0)
        def _():
            hand_map.wait_recv()
            put(map_out, slice(None), product(*chunk(map_in, slice(None)), own_high, own_low))

        for index in range(maps):
            whole_copy(0, index).start()
            whole_copy(1, index).start()

        @pl.when(x > 0)
        def _():
            hand_off.wait_recv()

            def even_offsets(index, carry):
                rows = rows_of(block, index)
                value = product(*chunk(off_in, rows), own_high, own_low)
                put(off_out, rows, plus(value, chunk(offset, rows)))
                return carry

            lax.fori_loop(0, columns // block, even_offsets, 0)

        for index in range(maps):
            forward(index)

    def take_whole(which):
        rows = pl.ds(pl.multiple_of(which * block, block), block)
        high, low = split(whole[which])
        whole_high[rows] = high
        whole_low[rows] = low

    whole[col] = map_out[...]
    take_whole(col)
    for index in range(maps // 2, maps):
        whole_copy(0, index).wait_recv()
    take_whole(down)
    for index in range(maps // 2):
        whole_copy(1, index).wait_recv()
    take_whole(up)
    for index in range(maps):
        whole_copy(2, index).wait_recv()
    take_whole(across)
    for kind in range(3):
        for index in range(maps):
            whole_copy(kind, index).wait_send()

    def z_copy(index):
        rows = rows_of(end_step, index)
        return remote(
            state.at[rows], z_in.at[rows], out_send.at[index], z_recv.at[index], at((z + 1) % planes, 3, 1)
        )

    def enter_copy(index):
        rows = rows_of(end_step, index)
        return remote(
            z_in.at[rows], x_in.at[rows], pass_send.at[index], x_recv.at[index], at(z, 0, 1)
        )

    def enter_back_copy(index):
        rows = rows_of(end_step, index)
        return remote(
            z_in.at[rows], x_in.at[rows], back_send.at[index], x_recv.at[index], at(z, 2, 1)
        )

    def back_copy(index):
        rows = rows_of(end_step, index)
        return remote(
            x_in.at[rows], x_in.at[rows], back_send.at[index], x_recv.at[index], at(z, x_before, 1)
        )

    def pass_copy(index):
        rows = rows_of(end_step, index)
        return remote(
            x_in.at[rows], x_in.at[rows], pass_send.at[index], x_recv.at[index], partner
        )

    def enter_core_copy(index):
        rows = rows_of(end_step, index)
        return remote(
            z_in.at[rows], x_in.at[rows], core_pass.at[index], x_recv.at[index], partner
        )

    @pl.when((core == 1) & (x == 3))
    def _():
        @pl.when(z == 0)
        def _():
            z_in[...] = jnp.zeros_like(z_in)
            state[...] = off_out[...]
            for index in range(ends):
                enter_copy(index).start()
                enter_back_copy(index).start()
                enter_core_copy(index).start()

        @pl.when(z > 0)
        def _():
            def z_sweep(index, carry):
                rows = rows_of(end_step, index)
                z_copy(index).wait_recv()
                enter_copy(index).start()
                enter_back_copy(index).start()
                enter_core_copy(index).start()
                value = product(*chunk(z_in, rows), whole_high, whole_low)
                put(state, rows, plus(value, chunk(off_out, rows)))

                @pl.when(z < planes - 1)
                def _():
                    z_copy(index).start()

                return carry

            def both_sweep(index, carry):
                @pl.when(z == 1)
                def _():
                    offsets(early + 2 * index, 2)

                z_sweep(2 * index, carry)
                return z_sweep(2 * index + 1, carry)

            lax.fori_loop(0, (ends - early) // 2, both_sweep, 0)

            @pl.when(z == 1)
            def _():
                hand_map.start()
                hand_off.start()

            lax.fori_loop(ends - early, ends, z_sweep, 0)

        @pl.when(z < planes - 1)
        def _():
            for index in range(ends):
                z_copy(index).wait_send()

        for index in range(ends):
            enter_copy(index).wait_send()
            enter_back_copy(index).wait_send()
            enter_core_copy(index).wait_send()

    def give(piece):
        rows = slice(piece * block, (piece + 1) * block)
        for part in range(2):
            out_ref[0, part, :, rows] = state[rows, part * width : (part + 1) * width].T

    @pl.when((core == 0) | (x < 3))
    def _():
        def x_sweep(index, carry):
            pass_copy(index).wait_recv()

            @pl.when(odd & (x == 2))
            def _():
                back_copy(index).start()

            @pl.when(odd)
            def _():
                pass_copy(index).start()

            rows = rows_of(end_step, index)
            value = product(*chunk(x_in, rows), whole_high, whole_low)
            put(state, rows, plus(value, chunk(off_out, rows)))
            return carry

        pieces = columns // block
        for piece in range(pieces):
            lax.fori_loop(piece * ends // pieces, (piece + 1) * ends // pieces, x_sweep, 0)
            give(piece)

        @pl.when(odd & (x == 2))
        def _():
            for index in range(ends):
                back_copy(index).wait_send()

        @pl.when(odd)
        def _():
            for index in range(ends):
                pass_copy(index).wait_send()

    @pl.when(odd & (x > 0))
    def _():
        hand_map.wait_send()
        hand_off.wait_send()

    @pl.when(core == 0)
    def _():
        for which in range(ROWS):
            even_map_copy(which, 0).wait_send()
            even_map_copy(which, 1).wait_send()
        even_offset_copy.wait_send()

    @pl.when(last)
    def _():
        for piece in range(columns // block):
            give(piece)


def local(planes, inverses, couplings, sources, counts):
    width, block = inverses.shape[2], inverses.shape[3]
    columns = sources.shape[3]
    map_chunks, end_chunks = 8, 16
    single, half = jnp.float32, jnp.bfloat16
    vmem, dma = pltpu.VMEM, pltpu.SemaphoreType.DMA
    held_map = vmem((width, 2 * width), half)
    rows_buffer = vmem((columns, 2 * width), single)
    map_buffer = vmem((block, 2 * width), single)
    in_hbm = pl.BlockSpec(memory_space=pltpu.HBM)
    in_vmem = pl.BlockSpec(memory_space=pltpu.VMEM)
    return pl.pallas_call(
        functools.partial(kernel, planes),
        out_shape=jax.ShapeDtypeStruct(sources.shape, single),
        in_specs=[in_hbm, in_hbm, in_hbm, pl.BlockSpec(memory_space=pltpu.SMEM)],
        out_specs=in_vmem,
        scratch_shapes=[
            vmem((ROWS, 2, width, block), single),
            vmem((ROWS, 2, width, block), single),
            vmem((2, width, columns), single),
            held_map,
            held_map,
            held_map,
            held_map,
            held_map,
            held_map,
            vmem((ROWS, block, 2 * width), single),
            vmem((ROWS, block, 2 * width), single),
            rows_buffer,
            rows_buffer,
            map_buffer,
            map_buffer,
            rows_buffer,
            rows_buffer,
            vmem((ROWS, block, 2 * width), single),
            held_map,
            held_map,
            rows_buffer,
            rows_buffer,
            rows_buffer,
            dma((3,)),
            dma((2, 6)),
            dma((2, 6)),
            dma((ROWS + 3, 2)),
            dma((ROWS + 3, 2)),
            dma((map_chunks,)),
            dma((map_chunks,)),
            dma((end_chunks,)),
            dma((end_chunks,)),
            dma((end_chunks,)),
            dma((end_chunks,)),
            dma((end_chunks,)),
            dma((end_chunks,)),
            dma((end_chunks,)),
            dma((3, map_chunks)),
            dma((3, map_chunks)),
            dma((end_chunks,)),
            pltpu.SemaphoreType.REGULAR,
        ],
        compiler_params=pltpu.CompilerParams(
            collective_id=0, has_side_effects=True, vmem_limit_bytes=40 * 2**20
        ),
    )(*(pltpu.with_memory_space_constraint(v, pltpu.HBM) for v in (inverses, couplings, sources)), counts)


def solution(mesh):
    placed = (
        P("chain", None, None, "col"),
        P("chain", None, None, "col"),
        P("chain", None, None, "col"),
        P("chain"),
    )
    return jax.shard_map(
        functools.partial(local, mesh.shape["chain"] // PLANE),
        mesh=mesh,
        in_specs=placed,
        out_specs=P("chain", None, None, "col"),
        check_vma=False,
    )
```
